256 devices in a mesh: dp: 16 (over x_hi, z), ctx: 16 (over y, x_lo, core).
Axes of the slice: x: 4 (x_hi: 2, x_lo: 2; x = x_hi * 2 + x_lo), y: 4, z: 8, core: 2. Of those that a mesh axis runs over, the one named last changes fastest.
Arguments:
- prompt_q: bfloat16 [16, 2048, 4096], P('dp', 'ctx'), may hold values from -260 to 260
- prompt_k: bfloat16 [16, 2048, 512], P('dp', 'ctx'), may hold values from -8 to 8
- prompt_v: bfloat16 [16, 2048, 512], P('dp', 'ctx'), may hold values from -12 to 12
- prompt_len: int32 [16], P('dp'), may hold values from 1024 to 2048
- resp_q: bfloat16 [16, 512, 4096], P('dp', 'ctx'), may hold values from -260 to 260
- resp_k: bfloat16 [16, 512, 512], P('dp', 'ctx'), may hold values from -6 to 6
- resp_v: bfloat16 [16, 512, 512], P('dp', 'ctx'), may hold values from -12 to 12
- resp_len: int32 [16, 32], P('dp', 'ctx'), may hold values from 1 to 16
- resp_resid: bfloat16 [16, 512, 4096], P('dp', 'ctx'), may hold values from -4 to 4
- norm_gain: float32 [4096], replicated, may hold values from 0.5 to 1.5
- gate_weight: bfloat16 [4096, 14336], P('dp', 'ctx'), may hold values from -0.09375 to 0.09375
- up_weight: bfloat16 [4096, 14336], P('dp', 'ctx'), may hold values from -0.09375 to 0.09375
Outputs:
- prompt_attn: bfloat16 [16, 2048, 4096], P('dp', 'ctx')
- resp_hidden: bfloat16 [16, 512, 14336], P('dp', None, 'ctx')
The draws below stay inside these ranges and needn't reach their ends.
All inputs are finite; a program needn't handle non-finite values.
Results may differ from the reference program's by a relative error of at most 0.012.
Values may be sent and summed in bfloat16 or wider, within the bound.
No kernel may reach another device: no remote copies, remote signals or barrier semaphores. Data moves between devices by JAX's collectives and lax.ppermute only.
A program may use at most 128 MiB of HBM per device.

```python
import jax
import jax.numpy as jnp
from jax import lax

QUERY_HEADS = 32
KEY_VALUE_HEADS = 4
HEAD_SIZE = 128
D = 4096
KVW = 512
FF = 14336
RLEN = 16
PROMPT_POSITIONS = 2048
RESP = 512
PROMPT_GROUPS = 16
N_CTX = 16


def marked_keys(key):
    base_offset = jax.random.fold_in(key, 11)
    key_matrix = jnp.clip(jax.random.normal(base_offset, (PROMPT_GROUPS, PROMPT_POSITIONS, KEY_VALUE_HEADS * HEAD_SIZE), jnp.float32), -6.0, 6.0)
    return key_matrix


def draw_prompt_k(key, part):
    key_matrix = marked_keys(key)
    return key_matrix.astype(jnp.bfloat16)


def draw_prompt_q(key, part):
    base_offset = jax.random.fold_in(key, 13)
    queries = 1.5 * jnp.clip(jax.random.normal(base_offset, (PROMPT_GROUPS, PROMPT_POSITIONS, QUERY_HEADS * HEAD_SIZE), jnp.float32), -6.0, 6.0)
    return queries.astype(jnp.bfloat16)


def draw_resp_q(key, part):
    base_offset = jax.random.fold_in(key, 14)
    queries = 1.5 * jnp.clip(jax.random.normal(base_offset, (PROMPT_GROUPS, RESP, QUERY_HEADS * HEAD_SIZE), jnp.float32), -6.0, 6.0)
    return queries.astype(jnp.bfloat16)


def touch_ends(values, rng, low, largest):
    place = [jax.random.randint(jax.random.fold_in(rng, axis), (), 0, length) for axis, length in enumerate(values.shape)]
    longest = values.shape.index(max(values.shape))
    neighbour = place[:longest] + [(place[longest] + 1) % values.shape[longest]] + place[longest + 1:]
    return values.at[tuple(place)].set(low).at[tuple(neighbour)].set(largest)


def shard_levels(rng, extent, cuts, least, top_value):
    def one(position, parts):
        draws = jax.random.uniform(jax.random.fold_in(jax.random.fold_in(rng, 6), position), (parts,), jnp.float32, least / len(cuts), top_value / len(cuts))
        return jnp.repeat(jnp.exp(draws), extent[position] // parts).reshape((-1,) + (1,) * (len(extent) - position - 1))

    level = one(*cuts[0])
    for cut in cuts[1:]:
        level = level * one(*cut)
    return level


def normal_values(key, extent, width, most, split=(), kind=jnp.bfloat16):
    values = width * jax.random.normal(key, extent, jnp.float32)
    if split:
        values = values * shard_levels(key, extent, split, -0.22, 0.18)
    return jnp.clip(values, -most, most).astype(kind)


def setup_inputs(seed: int = 0) -> dict:
    key_of = jax.random.split(jax.random.key(seed), 13)
    prompt_q = draw_prompt_q(jax.random.fold_in(key_of[12], 71), 0)
    prompt_k = draw_prompt_k(jax.random.fold_in(key_of[12], 71), 0)
    prompt_v = normal_values(key_of[2], (PROMPT_GROUPS, PROMPT_POSITIONS, KVW), 2.0, 12.0, ((0, 16), (1, 16)))
    prompt_len = touch_ends(jax.random.randint(key_of[3], (PROMPT_GROUPS,), PROMPT_POSITIONS // 2, PROMPT_POSITIONS + 1), jax.random.fold_in(key_of[3], 1), PROMPT_POSITIONS // 2, PROMPT_POSITIONS).astype(jnp.int32)
    resp_q = draw_resp_q(jax.random.fold_in(key_of[12], 71), 0)
    resp_k = normal_values(key_of[5], (PROMPT_GROUPS, RESP, KVW), 1.0, 6.0, ((0, 16), (1, 16)))
    resp_v = normal_values(key_of[6], (PROMPT_GROUPS, RESP, KVW), 2.0, 12.0, ((0, 16), (1, 16)))
    resp_len = touch_ends(jax.random.randint(key_of[7], (PROMPT_GROUPS, 2 * N_CTX), 1, RLEN + 1), jax.random.fold_in(key_of[7], 1), 1, RLEN).astype(jnp.int32)
    resp_resid = normal_values(key_of[8], (PROMPT_GROUPS, RESP, D), 0.5, 4.0, ((0, 16), (1, 16)))
    norm_gain = jnp.clip(1.0 + 0.1 * jax.random.normal(key_of[9], (D,), jnp.float32), 0.5, 1.5)
    gate_weight = normal_values(key_of[10], (D, FF), D ** -0.5, 0.09375, ((0, 16), (1, 16)))
    up_weight = normal_values(key_of[11], (D, FF), D ** -0.5, 0.09375, ((0, 16), (1, 16)))
    return dict(prompt_q=prompt_q, prompt_k=prompt_k, prompt_v=prompt_v, prompt_len=prompt_len, resp_q=resp_q, resp_k=resp_k, resp_v=resp_v, resp_len=resp_len, resp_resid=resp_resid, norm_gain=norm_gain, gate_weight=gate_weight, up_weight=up_weight)


def to_heads(token_rows):
    group_count = token_rows.shape[0]
    return token_rows.reshape(group_count, KEY_VALUE_HEADS, QUERY_HEADS // KEY_VALUE_HEADS, HEAD_SIZE).transpose(1, 2, 0, 3).reshape(KEY_VALUE_HEADS, QUERY_HEADS // KEY_VALUE_HEADS * group_count, HEAD_SIZE)

def from_heads(head_rows, group_count):
    return head_rows.reshape(KEY_VALUE_HEADS, QUERY_HEADS // KEY_VALUE_HEADS, group_count, HEAD_SIZE).transpose(2, 0, 1, 3).reshape(group_count, QUERY_HEADS * HEAD_SIZE)

def key_heads(token_rows):
    return token_rows.reshape(token_rows.shape[0], KEY_VALUE_HEADS, HEAD_SIZE).transpose(1, 0, 2)

def attend(queries, key_matrix, values, visible_mask):
    grouped_heads = jnp.tile(visible_mask, (QUERY_HEADS // KEY_VALUE_HEADS, 1))[None]
    scores = jnp.einsum('kqd,ktd->kqt', queries.astype(jnp.float32), key_matrix.astype(jnp.float32)) * HEAD_SIZE ** (-0.5)
    scores = jnp.where(grouped_heads, scores, -1e+30)
    top = lax.optimization_barrier(jnp.max(scores, axis=-1, keepdims=True))
    weights = jnp.where(grouped_heads, jnp.exp(scores - top), 0.0)
    total = lax.optimization_barrier(jnp.sum(weights, axis=-1))
    rounded = lax.optimization_barrier(weights.astype(jnp.bfloat16))
    mixed = jnp.einsum('kqt,ktd->kqd', rounded.astype(jnp.float32), values.astype(jnp.float32))
    return mixed / total[..., None]

def one_group(inputs):
    pq, pk, pv, plen, rq, rk, rv, rlen, resid, gain, gate_weight, up_weight = inputs
    key_matrix = key_heads(pk)
    values = key_heads(pv)
    key_position = jnp.arange(PROMPT_POSITIONS, dtype=jnp.int32)
    attention_block = min(PROMPT_POSITIONS, 512)

    def prompt_block(index):
        start = index * attention_block
        token_rows = lax.dynamic_slice_in_dim(pq, start, attention_block, 0)
        qpos = start + jnp.arange(attention_block, dtype=jnp.int32)
        visible_mask = (key_position[None, :] <= qpos[:, None]) & (key_position[None, :] < plen)
        out = attend(to_heads(token_rows), key_matrix, values, visible_mask)
        return from_heads(out, attention_block).astype(jnp.bfloat16)
    prompt_out = lax.map(prompt_block, jnp.arange(PROMPT_POSITIONS // attention_block, dtype=jnp.int32)).reshape(PROMPT_POSITIONS, QUERY_HEADS * HEAD_SIZE)
    token_rows = jnp.arange(RESP, dtype=jnp.int32)
    slot_r = token_rows // RLEN
    place_r = token_rows % RLEN
    limit = rlen[slot_r]
    prompt_vis = jnp.broadcast_to((key_position < plen)[None, :], (RESP, PROMPT_POSITIONS))
    own_vis = (slot_r[:, None] == slot_r[None, :]) & (place_r[None, :] <= place_r[:, None]) & (place_r[None, :] < limit[None, :])
    visible_mask = jnp.concatenate([prompt_vis, own_vis], axis=1)
    all_keys = jnp.concatenate([key_matrix, key_heads(rk)], axis=1)
    all_values = jnp.concatenate([values, key_heads(rv)], axis=1)
    resp_attn = from_heads(attend(to_heads(rq), all_keys, all_values, visible_mask), RESP).astype(jnp.bfloat16)
    stream = resid.astype(jnp.float32) + resp_attn.astype(jnp.float32)
    scale = lax.rsqrt(lax.optimization_barrier(jnp.mean(stream * stream, axis=-1, keepdims=True)) + 1e-05)
    normed = (stream * scale * gain).astype(jnp.bfloat16)
    gate = jnp.dot(normed, gate_weight, preferred_element_type=jnp.float32)
    up = jnp.dot(normed, up_weight, preferred_element_type=jnp.float32)
    hidden = (jax.nn.silu(gate) * up).astype(jnp.bfloat16)
    return (prompt_out, hidden)

def reference(prompt_q, prompt_k, prompt_v, prompt_len, resp_q, resp_k, resp_v, resp_len, resp_resid, norm_gain, gate_weight, up_weight):
    outs = []
    hiddens = []
    for group in range(PROMPT_GROUPS):
        prompt_out, hidden = one_group((prompt_q[group], prompt_k[group], prompt_v[group], prompt_len[group], resp_q[group], resp_k[group], resp_v[group], resp_len[group], resp_resid[group], norm_gain, gate_weight, up_weight))
        outs.append(prompt_out)
        hiddens.append(hidden)
    return (jnp.stack(outs), jnp.stack(hiddens))
```

```python
import functools

import jax
import jax.numpy as jnp
from jax import lax
from jax.experimental import pallas as pl
from jax.experimental.pallas import tpu as pltpu
from jax.sharding import Mesh
from jax.sharding import PartitionSpec as P

KEY_VALUE_HEADS = 4
GROUP = 8
HEAD_SIZE = 128
RLEN = 16
X = ("xh", "xl")
CTX = ("y", "xl", "c")
DP = ("xh", "z")
TO_LOG2 = 1.4426950408889634 * HEAD_SIZE**-0.5
HIDDEN = -1e30
NEAR = (0, -1, 1, -2, 2)
FAR = (-3, 3, 4)
VMEM = pl.BlockSpec(memory_space=pltpu.VMEM)
SMEM = pl.BlockSpec(memory_space=pltpu.SMEM)


def params(limit):
    return pltpu.CompilerParams(vmem_limit_bytes=limit << 20)


def cost(flops, moved, exps=0):
    return pl.CostEstimate(flops=flops, bytes_accessed=moved, transcendentals=exps)


def shift(a, axis, by):
    n = lax.axis_size(axis)
    return lax.ppermute(a, axis, [(i, (i + by) % n) for i in range(n)])


def halves(a, axis):
    n = a.shape[axis] // 2
    return lax.slice_in_dim(a, 0, n, axis=axis), lax.slice_in_dim(a, n, 2 * n, axis=axis)


def ring4(a, axis):
    low = shift(a, axis, 1)
    high = shift(a, axis, -1)
    far_a = shift(halves(low, 0)[0], axis, 1)
    far_b = shift(halves(high, 0)[1], axis, -1)
    return [a, low, high, far_a, far_b]


RING = (0, -1, 1, 2)


def pack_kernel(ids, gate, up, mine, theirs):
    def pack(half, out):
        start, tail = (0, 384) if half == 0 else (512, 448)
        for b in range(3):
            at = start + 128 * b
            out[:, 256 * b : 256 * b + 128] = gate[:, at : at + 128]
            out[:, 256 * b + 128 : 256 * b + 256] = up[:, at : at + 128]
        out[:, 768:832] = gate[:, tail : tail + 64]
        out[:, 832:896] = up[:, tail : tail + 64]

    @pl.when(ids[0] == 0)
    def _():
        pack(0, mine)
        pack(1, theirs)

    @pl.when(ids[0] != 0)
    def _():
        pack(1, mine)
        pack(0, theirs)


def pack(ids, gate, up):
    shape = jax.ShapeDtypeStruct(gate.shape, gate.dtype)
    return pl.pallas_call(
        pack_kernel,
        out_shape=(shape, shape),
        in_specs=[SMEM, VMEM, VMEM],
        out_specs=(VMEM, VMEM),
        compiler_params=params(8),
        cost_estimate=cost(10**6, 2 * 2 * gate.size * 2),
        name="pack",
    )(ids, gate, up)


def ring8(shard):
    pieces = {0: [shard]}
    low = high = shard
    for d in (1, 2, 3):
        low, high = shift(low, "z", 1), shift(high, "z", -1)
        pieces[-d], pieces[d] = [low], [high]
    pieces[4] = [shift(halves(low, 0)[0], "z", 1), shift(halves(high, 0)[1], "z", -1)]
    return pieces


def resp_kernel(ids, *refs):
    blocks, (q, rk, rv, resid, gain, kv, left, right, attn) = refs[:20], refs[20:]
    y, xl, c, limit, len0, len1 = (ids[i] for i in (2, 3, 4, 5, 6, 7))
    for side in range(2):
        cc = c if side == 0 else 1 - c
        for beside in range(2):
            xx = xl if beside == 0 else 1 - xl
            at = side * 10 + beside * 5
            for d, parts in zip(RING, ([0], [1], [2], [3, 4])):
                yy = lax.rem(y + d + 4, 4)
                row = ((yy * 2 + xx) * 2 + cc) * 128
                for part in parts:
                    ref = blocks[at + part]
                    n = ref.shape[0]
                    kv[pl.ds(pl.multiple_of(row, 64), n), :] = ref[...]
                    row = row + n
    rows = GROUP * 32
    r = lax.rem(lax.broadcasted_iota(jnp.int32, (rows, 32), 0), 32)
    t = lax.broadcasted_iota(jnp.int32, (rows, 32), 1)
    slot_t, place_t = t // RLEN, lax.rem(t, RLEN)
    own = (
        (r // RLEN == slot_t)
        & (place_t <= lax.rem(r, RLEN))
        & (place_t < jnp.where(slot_t == 0, len0, len1))
    )
    block = 512
    column = lax.broadcasted_iota(jnp.int32, (rows, block), 1)
    for h in range(KEY_VALUE_HEADS):
        lanes = slice(h * HEAD_SIZE, (h + 1) * HEAD_SIZE)
        heads = [(h * GROUP + g) * HEAD_SIZE for g in range(GROUP)]
        qs = jnp.concatenate([q[:, at : at + HEAD_SIZE] for at in heads], axis=0)
        dims = (((1,), (1,)), ((), ()))
        s = lax.dot_general(qs, rk[:, lanes], dims, preferred_element_type=jnp.float32)
        s = jnp.where(own, s, HIDDEN)
        top = jnp.max(s, axis=1, keepdims=True)
        w = jnp.exp2((s - top) * TO_LOG2)
        total = jnp.sum(w, axis=1, keepdims=True)
        mixed = jnp.dot(w.astype(jnp.bfloat16), rv[:, lanes], preferred_element_type=jnp.float32)
        for b in range(4):
            keys = kv[b * block : (b + 1) * block, lanes]
            values = kv[b * block : (b + 1) * block, 512 + h * HEAD_SIZE : 512 + (h + 1) * HEAD_SIZE]
            s = lax.dot_general(qs, keys, dims, preferred_element_type=jnp.float32)
            if b >= 2:
                s = jnp.where(column < limit - b * block, s, HIDDEN)
            new = jnp.maximum(top, jnp.max(s, axis=1, keepdims=True))
            w = jnp.exp2((s - new) * TO_LOG2)
            factor = jnp.exp2((top - new) * TO_LOG2)
            total = total * factor + jnp.sum(w, axis=1, keepdims=True)
            mixed = mixed * factor + jnp.dot(
                w.astype(jnp.bfloat16), values, preferred_element_type=jnp.float32
            )
            top = new
        out = (mixed / total).astype(jnp.bfloat16)
        for g, at in enumerate(heads):
            attn[:, at : at + HEAD_SIZE] = out[g * 32 : (g + 1) * 32, :]
    stream = resid[...].astype(jnp.float32) + attn[...].astype(jnp.float32)
    scale = lax.rsqrt(jnp.mean(stream * stream, axis=1, keepdims=True) + 1e-05)
    normed = (stream * scale * gain[...]).astype(jnp.bfloat16)
    left[...] = normed[:, :2048]
    right[...] = normed[:, 2048:]


def resp_attention(ids, blocks, q, rk, rv, resid, gain):
    half = jax.ShapeDtypeStruct((32, 2048), jnp.bfloat16)
    return pl.pallas_call(
        resp_kernel,
        out_shape=(jax.ShapeDtypeStruct((2048, 1024), jnp.bfloat16), half, half),
        in_specs=[SMEM] + [VMEM] * 25,
        out_specs=(VMEM, VMEM, VMEM),
        scratch_shapes=[pltpu.VMEM((32, 4096), jnp.bfloat16)],
        compiler_params=params(24),
        cost_estimate=cost(4 * 1024 * 2080 * 128, 9 << 20, 1024 * 2080),
        name="resp_attention",
    )(ids, *blocks, q, rk, rv, resid, gain)


def prompt_kernel(ids, q, keys, values, out, *, block):
    here = (ids[2] * 2 + ids[3]) * 2 + ids[4]
    limit = ids[5]
    rows = GROUP * 128
    qs = jnp.concatenate([q[:, g * HEAD_SIZE : (g + 1) * HEAD_SIZE] for g in range(GROUP)], axis=0)
    place = lax.rem(lax.broadcasted_iota(jnp.int32, (rows, block), 0), 128)
    ends = jnp.minimum(here * 128 + place + 1, limit)
    gap = lax.broadcasted_iota(jnp.int32, (rows, block), 1) - ends
    last = jnp.minimum((here + 1) * 128, limit)

    def step(b, carry):
        top, total, mixed = carry
        at = pl.multiple_of(b * block, block)
        s = lax.dot_general(
            qs, keys[pl.ds(at, block), :], (((1,), (1,)), ((), ())), preferred_element_type=jnp.float32
        )
        s = jnp.where(gap < -at, s, HIDDEN)
        new = jnp.maximum(top, jnp.max(s, axis=1, keepdims=True))
        w = jnp.exp2((s - new) * TO_LOG2)
        factor = jnp.exp2((top - new) * TO_LOG2)
        total = total * factor + jnp.sum(w, axis=1, keepdims=True)
        mixed = mixed * factor + jnp.dot(
            w.astype(jnp.bfloat16), values[pl.ds(at, block), :], preferred_element_type=jnp.float32
        )
        return new, total, mixed

    start = (
        jnp.full((rows, 1), HIDDEN, jnp.float32),
        jnp.zeros((rows, 1), jnp.float32),
        jnp.zeros((rows, HEAD_SIZE), jnp.float32),
    )
    _, total, mixed = lax.fori_loop(0, (last + block - 1) // block, step, start)
    done = (mixed / total).astype(jnp.bfloat16)
    for g in range(GROUP):
        out[:, g * HEAD_SIZE : (g + 1) * HEAD_SIZE] = done[g * 128 : (g + 1) * 128, :]


def prompt_attention(ids, q, kv, first, count):
    return pl.pallas_call(
        functools.partial(prompt_kernel, block=512),
        out_shape=jax.ShapeDtypeStruct((128, 1024 * count), jnp.bfloat16),
        grid=(count,),
        in_specs=[
            SMEM,
            pl.BlockSpec((128, 1024), lambda h: (0, h + first)),
            pl.BlockSpec((2048, 128), lambda h: (0, h + first)),
            pl.BlockSpec((2048, 128), lambda h: (0, h + first + KEY_VALUE_HEADS)),
        ],
        out_specs=pl.BlockSpec((128, 1024), lambda h: (0, h)),
        compiler_params=params(32),
        cost_estimate=cost(count * 4 * 1024 * 2048 * 128 * 3, count << 20, count * 1024 * 2048),
        name="prompt_attention",
    )(ids, q, kv, kv)


def rows_kernel(ids, *refs):
    lefts, rights, near, far = refs[:10], refs[10:20], refs[20], refs[21]
    xh, z, y, xl, c = (ids[i] for i in range(5))
    x = xh * 2 + xl

    def place(ref, side, outer_by_x):
        pass

    def put(ref, first, count, outer, cc, outer_is_y, use_second):
        def lanes_of(kz, _):
            d = lax.rem(kz - z + 8, 8)
            slot = jnp.where(d == 0, 0, jnp.where(d == 4, 7, jnp.where(d < 4, 2 * d, 2 * (8 - d) - 1)))
            lane = pl.multiple_of((slot * 2 + use_second) * 256, 256)
            src = pl.ds(pl.multiple_of(kz * 256, 256), 256)
            for n in range(count):
                inner = RING[first + n]
                if outer_is_y:
                    yy, xx = outer, lax.rem(x + inner + 4, 4)
                else:
                    yy, xx = lax.rem(y + inner + 4, 4), outer
                row = (xx // 2) * 512 + yy * 128 + lax.rem(xx, 2) * 64 + cc * 32
                dst = pl.ds(pl.multiple_of(row, 32), 32)
                value = ref[n * 32 : (n + 1) * 32, src]

                @pl.when(slot < 5)
                def _():
                    near[dst, pl.ds(lane, 256)] = value

                @pl.when(slot >= 5)
                def _():
                    far[dst, pl.ds(pl.multiple_of(lane - 2560, 256), 256)] = value

            return 0

        lax.fori_loop(0, 8, lanes_of, 0)

    for refs5, outer_is_y in ((lefts, True), (rights, False)):
        second = jnp.where(xh == 0, 0, 1) if outer_is_y else jnp.where(xh == 0, 1, 0)
        base = y if outer_is_y else x
        for side in range(2):
            cc = c if side == 0 else 1 - c
            for part, d, first, count in ((0, 0, 0, 4), (1, -1, 0, 4), (2, 1, 0, 4), (3, 2, 0, 2), (4, 2, 2, 2)):
                put(refs5[side * 5 + part], first, count, lax.rem(base + d + 4, 4), cc, outer_is_y, second)


def assemble_rows(ids, lefts, rights):
    return pl.pallas_call(
        rows_kernel,
        out_shape=(
            jax.ShapeDtypeStruct((1024, 2560), jnp.bfloat16),
            jax.ShapeDtypeStruct((1024, 1536), jnp.bfloat16),
        ),
        in_specs=[SMEM] + [VMEM] * 20,
        out_specs=(VMEM, VMEM),
        compiler_params=params(24),
        cost_estimate=cost(10**6, 16 << 20),
        name="assemble_rows",
    )(ids, *lefts, *rights)


def near_kernel(a, *refs):
    slices, out, w = refs[:-2], refs[-2], refs[-1]
    for i, ref in enumerate(slices):
        w[i * 256 : (i + 1) * 256, :] = ref[...]

    def tile(i, _):
        rows = pl.ds(pl.multiple_of(i * 256, 256), 256)
        out[rows, :] = jnp.dot(a[rows, :], w[...], preferred_element_type=jnp.float32)
        return 0

    lax.fori_loop(0, 4, tile, 0)


def near_product(a, slices):
    return pl.pallas_call(
        near_kernel,
        out_shape=jax.ShapeDtypeStruct((1024, 896), jnp.float32),
        in_specs=[VMEM] * (1 + len(slices)),
        out_specs=VMEM,
        scratch_shapes=[pltpu.VMEM((2560, 896), jnp.bfloat16)],
        compiler_params=params(28),
        cost_estimate=cost(2 * 1024 * 2560 * 896, 14 << 20),
        name="near_product",
    )(a, *slices)


def far_kernel(ids, a, acc, *refs):
    slices, mine, theirs, w = refs[:-3], refs[-3], refs[-2], refs[-1]
    at = 0
    for ref in slices:
        n = ref.shape[0]
        w[at : at + n, :] = ref[...]
        at += n

    def tile(i, _):
        rows = pl.ds(pl.multiple_of(i * 128, 128), 128)
        both = acc[rows, :] + jnp.dot(a[rows, :], w[...], preferred_element_type=jnp.float32)

        def hidden(gate, up):
            return (gate / (1.0 + jnp.exp(-gate)) * up).astype(jnp.bfloat16)

        parts = [hidden(both[:, b : b + 128], both[:, b + 128 : b + 256]) for b in (0, 256, 512)]
        tail = hidden(both[:, 768:832], both[:, 832:896])
        dst = pl.ds(pl.multiple_of(lax.rem(i, 4) * 128, 128), 128)

        def put(out):
            for b in range(3):
                out[dst, b * 128 : (b + 1) * 128] = parts[b]
            out[dst, 384:448] = tail

        @pl.when(i // 4 == ids[0])
        def _():
            put(mine)

        @pl.when(i // 4 != ids[0])
        def _():
            put(theirs)

        return 0

    lax.fori_loop(0, 8, tile, 0)


def far_product(ids, a, acc, slices):
    half = jax.ShapeDtypeStruct((512, 448), jnp.bfloat16)
    return pl.pallas_call(
        far_kernel,
        out_shape=(half, half),
        in_specs=[SMEM] + [VMEM] * (2 + len(slices)),
        out_specs=(VMEM, VMEM),
        scratch_shapes=[pltpu.VMEM((1536, 896), jnp.bfloat16)],
        compiler_params=params(28),
        cost_estimate=cost(2 * 1024 * 1536 * 896, 12 << 20),
        name="far_product",
    )(ids, a, acc, *slices)


def gather_rows(left, right):
    by_x = jnp.concatenate(ring4(left, X), axis=0)
    by_y = jnp.concatenate(ring4(right, "y"), axis=0)
    lefts = ring4(by_x, "y")
    rights = ring4(by_y, X)
    return lefts + [shift(a, "c", 1) for a in lefts], rights + [shift(a, "c", 1) for a in rights]


def local(
    prompt_q,
    prompt_k,
    prompt_v,
    prompt_len,
    resp_q,
    resp_k,
    resp_v,
    resp_len,
    resp_resid,
    norm_gain,
    gate_weight,
    up_weight,
):
    places = [lax.axis_index(a).astype(jnp.int32) for a in ("xh", "z", "y", "xl", "c")]
    ids = jnp.stack(places + [prompt_len[0], resp_len[0, 0], resp_len[0, 1]])
    xh = places[0]

    own = jnp.concatenate([prompt_k[0], prompt_v[0]], axis=1)
    beside = shift(own, "xl", 1)
    blocks = ring4(own, "y") + ring4(beside, "y")
    blocks = blocks + [shift(a, "c", 1) for a in blocks]

    mine, theirs = pack(ids, gate_weight, up_weight)
    first = ring8(mine)
    second = ring8(shift(theirs, "xh", 1))

    kv, left, right = resp_attention(
        ids, blocks, resp_q[0], resp_k[0], resp_v[0], resp_resid[0], norm_gain.reshape(1, -1)
    )
    lefts, rights = gather_rows(left, right)
    prompts = [prompt_attention(ids, prompt_q[0], kv, h, 1) for h in range(KEY_VALUE_HEADS)]
    prompt_out = jnp.concatenate(prompts, axis=1)

    near, far = assemble_rows(ids, lefts, rights)
    acc = near_product(near, [a for d in NEAR for s in (first, second) for a in s[d]])
    done, away = far_product(ids, far, acc, [a for d in FAR for s in (first, second) for a in s[d]])
    got = shift(away, "xh", 1)
    zero = jnp.where(xh == 0, done, got)
    one = jnp.where(xh == 0, got, done)
    hidden = jnp.concatenate([zero, one[:, 384:], one[:, :384]], axis=1)
    return (prompt_out[None], hidden[None])


def solution(mesh):
    finer = Mesh(mesh.devices.reshape(2, 8, 4, 2, 2), ("xh", "z", "y", "xl", "c"))
    return jax.shard_map(
        local,
        mesh=finer,
        in_specs=(
            P(DP, CTX, None),
            P(DP, CTX, None),
            P(DP, CTX, None),
            P(DP),
            P(DP, CTX, None),
            P(DP, CTX, None),
            P(DP, CTX, None),
            P(DP, CTX),
            P(DP, CTX, None),
            P(),
            P(DP, CTX),
            P(DP, CTX),
        ),
        out_specs=(P(DP, CTX, None), P(DP, None, CTX)),
        check_vma=False,
    )
```

```python
import functools

import jax
import jax.numpy as jnp
from jax import lax
from jax.experimental import pallas as pl
from jax.experimental.pallas import tpu as pltpu
from jax.sharding import Mesh
from jax.sharding import PartitionSpec as P

KEY_VALUE_HEADS = 4
GROUP = 8
HEAD_SIZE = 128
RLEN = 16
CTX = ("y", "xl", "c")
DP = ("xh", "z")
TO_LOG2 = 1.4426950408889634 * HEAD_SIZE**-0.5
HIDDEN = -1e30
NEAR = (0, -1, 1, -2, 2)
FAR = (-3, 3, 4)
VMEM = pl.BlockSpec(memory_space=pltpu.VMEM)
SMEM = pl.BlockSpec(memory_space=pltpu.SMEM)


def params(limit):
    return pltpu.CompilerParams(vmem_limit_bytes=limit << 20)


def cost(flops, moved, exps=0):
    return pl.CostEstimate(flops=flops, bytes_accessed=moved, transcendentals=exps)


def shift(a, axis, by):
    n = lax.axis_size(axis)
    return lax.ppermute(a, axis, [(i, (i + by) % n) for i in range(n)])


def halves(a, axis):
    n = a.shape[axis] // 2
    return lax.slice_in_dim(a, 0, n, axis=axis), lax.slice_in_dim(a, n, 2 * n, axis=axis)


def ring4(a, axes, pairs):
    low = lax.ppermute(a, axes, pairs(1))
    high = lax.ppermute(a, axes, pairs(-1))
    far_a = lax.ppermute(halves(low, 0)[0], axes, pairs(1))
    far_b = lax.ppermute(halves(high, 0)[1], axes, pairs(-1))
    return [a, low, high, jnp.concatenate([far_a, far_b], axis=0)]


def shared(pieces):
    return pieces + [shift(a, "c", 1) for a in pieces]


def along_y(by):
    return [(i, (i + by) % 4) for i in range(4)]


def crossed(x_first, by):
    def flat(x, y, c):
        return ((x // 2 * 4 + y) * 2 + x % 2) * 2 + c

    out = []
    for x in range(4):
        for y in range(4):
            for c in range(2):
                to = ((x + by) % 4, y) if (c == 0) == x_first else (x, (y + by) % 4)
                out.append((flat(x, y, c), flat(*to, c)))
    return out


RING = (0, -1, 1, 2)


def places():
    return [lax.axis_index(a).astype(jnp.int32) for a in ("xh", "z", "y", "xl", "c")]


def pack_kernel(gate, up, mine, theirs):
    xh = places()[0]

    def pack(half, out):
        start, tail = (0, 384) if half == 0 else (512, 448)
        for b in range(3):
            at = start + 128 * b
            out[:, 256 * b : 256 * b + 128] = gate[:, at : at + 128]
            out[:, 256 * b + 128 : 256 * b + 256] = up[:, at : at + 128]
        out[:, 768:832] = gate[:, tail : tail + 64]
        out[:, 832:896] = up[:, tail : tail + 64]

    @pl.when(xh == 0)
    def _():
        pack(0, mine)
        pack(1, theirs)

    @pl.when(xh != 0)
    def _():
        pack(1, mine)
        pack(0, theirs)


def pack(gate, up):
    shape = jax.ShapeDtypeStruct(gate.shape, gate.dtype)
    return pl.pallas_call(
        pack_kernel,
        out_shape=(shape, shape),
        in_specs=[VMEM, VMEM],
        out_specs=(VMEM, VMEM),
        compiler_params=params(8),
        cost_estimate=cost(10**9, 2 * 2 * gate.size * 2),
        name="pack",
    )(gate, up)


def ring8(shard):
    pieces = {0: [shard]}
    low = high = shard
    for d in (1, 2, 3):
        low = shift(low, "z", 1)
        high = shift(high, "z", -1)
        pieces[-d], pieces[d] = [low], [high]
    return pieces


def farthest(pieces, after):
    low, high, _ = lax.optimization_barrier((pieces[-3][0], pieces[3][0], after))
    low, high = halves(low, 0)[0], halves(high, 0)[1]
    return [shift(low, "z", 1), shift(high, "z", -1)]


ROWS = (((1,), (1,)), ((), ()))
COLUMNS = (((0,), (0,)), ((), ()))


def weigh(s, values, top, total, mixed):
    new = jnp.maximum(top, jnp.max(s, axis=0, keepdims=True))
    w = jnp.exp2((s - new) * TO_LOG2)
    factor = jnp.exp2((top - new) * TO_LOG2)
    total = total * factor + jnp.sum(w, axis=0, keepdims=True)
    product = lax.dot_general(
        values, w.astype(jnp.bfloat16), COLUMNS, preferred_element_type=jnp.float32
    )
    return new, total, mixed * factor + product


def resp_kernel(plen, rlen, *refs):
    blocks, (q, rk, rv, resid, gain, kv, out, attn) = refs[:8], refs[8:]
    _, z, y, xl, c = places()
    limit, len0, len1 = plen[0], rlen[0, 0], rlen[0, 1]
    for side in range(2):
        cc = c if side == 0 else 1 - c
        for part, d in enumerate(RING):
            ref = blocks[side * 4 + part]
            yy = lax.rem(y + d + 4, 4)
            for beside in range(2):
                xx = xl if beside == 0 else 1 - xl
                row = pl.multiple_of(((yy * 2 + xx) * 2 + cc) * 128, 128)
                kv[pl.ds(row, 128), :] = ref[beside * 128 : (beside + 1) * 128, :]
    columns = GROUP * 32
    r = lax.rem(lax.broadcasted_iota(jnp.int32, (32, columns), 1), 32)
    t = lax.broadcasted_iota(jnp.int32, (32, columns), 0)
    slot_t, place_t = t // RLEN, lax.rem(t, RLEN)
    own = (
        (r // RLEN == slot_t)
        & (place_t <= lax.rem(r, RLEN))
        & (place_t < jnp.where(slot_t == 0, len0, len1))
    )
    block = 512
    row = lax.broadcasted_iota(jnp.int32, (block, columns), 0)

    def head(h, _):
        lanes = pl.ds(pl.multiple_of(h * HEAD_SIZE, HEAD_SIZE), HEAD_SIZE)
        behind = pl.ds(pl.multiple_of(512 + h * HEAD_SIZE, HEAD_SIZE), HEAD_SIZE)
        heads = [
            pl.ds(pl.multiple_of((h * GROUP + g) * HEAD_SIZE, HEAD_SIZE), HEAD_SIZE) for g in range(GROUP)
        ]
        qs = jnp.concatenate([q[:, at] for at in heads], axis=0)
        s = lax.dot_general(rk[:, lanes], qs, ROWS, preferred_element_type=jnp.float32)
        carry = weigh(
            jnp.where(own, s, HIDDEN),
            rv[:, lanes],
            jnp.full((1, columns), HIDDEN, jnp.float32),
            jnp.zeros((1, columns), jnp.float32),
            jnp.zeros((HEAD_SIZE, columns), jnp.float32),
        )

        def step(b, carry):
            keys = pl.ds(pl.multiple_of(b * block, block), block)
            s = lax.dot_general(kv[keys, lanes], qs, ROWS, preferred_element_type=jnp.float32)
            s = jnp.where(row < limit - b * block, s, HIDDEN)
            return weigh(s, kv[keys, behind], *carry)

        carry = lax.fori_loop(0, 2048 // block, step, carry)
        _, total, mixed = carry
        done = (mixed / total).T.astype(jnp.bfloat16)
        for g, at in enumerate(heads):
            attn[:, at] = done[g * 32 : (g + 1) * 32, :]
        return 0

    lax.fori_loop(0, KEY_VALUE_HEADS, head, 0)
    stream = resid[...].astype(jnp.float32) + attn[...].astype(jnp.float32)
    scale = lax.rsqrt(jnp.mean(stream * stream, axis=1, keepdims=True) + 1e-05)
    normed = (stream * scale * gain[...]).astype(jnp.bfloat16)
    for half in range(2):
        for k in range(8):
            d = lax.rem(k - z + 8, 8)
            slot = jnp.where(d == 0, 0, jnp.where(d == 4, 7, jnp.where(d < 4, 2 * d, 2 * (8 - d) - 1)))
            lane = pl.multiple_of(half * 2048 + slot * 256, 256)
            out[:, pl.ds(lane, 256)] = normed[:, half * 2048 + k * 256 : half * 2048 + (k + 1) * 256]


def resp_attention(plen, rlen, blocks, q, rk, rv, resid, gain):
    return pl.pallas_call(
        resp_kernel,
        out_shape=(
            jax.ShapeDtypeStruct((2048, 1024), jnp.bfloat16),
            jax.ShapeDtypeStruct((32, 4096), jnp.bfloat16),
        ),
        in_specs=[SMEM, SMEM] + [VMEM] * 13,
        out_specs=(VMEM, VMEM),
        scratch_shapes=[pltpu.VMEM((32, 4096), jnp.bfloat16)],
        compiler_params=params(24),
        cost_estimate=cost(4 * 1024 * 2080 * 128, 9 << 20, 1024 * 2080),
        name="resp_attention",
    )(plen, rlen, *blocks, q, rk, rv, resid, gain)


def prompt_kernel(plen, q, keys, values, *refs, block):
    out = refs[-1]
    _, _, y, xl, c = places()
    here = (y * 2 + xl) * 2 + c
    limit = plen[0]
    some = GROUP // 2
    columns = some * 128
    place = lax.rem(lax.broadcasted_iota(jnp.int32, (1, columns), 1), 128)
    ends = jnp.minimum(here * 128 + place + 1, limit)
    row = lax.broadcasted_iota(jnp.int32, (block, columns), 0)
    last = jnp.minimum((here + 1) * 128, limit)

    def half(i, _):
        heads = [
            pl.ds(pl.multiple_of((i * some + g) * HEAD_SIZE, HEAD_SIZE), HEAD_SIZE) for g in range(some)
        ]
        qs = jnp.concatenate([q[:, at] for at in heads], axis=0)

        def step(b, carry):
            at = pl.multiple_of(b * block, block)
            s = lax.dot_general(keys[pl.ds(at, block), :], qs, ROWS, preferred_element_type=jnp.float32)
            s = jnp.where(row < ends - at, s, HIDDEN)
            return weigh(s, values[pl.ds(at, block), :], *carry)

        carry = (
            jnp.full((1, columns), HIDDEN, jnp.float32),
            jnp.zeros((1, columns), jnp.float32),
            jnp.zeros((HEAD_SIZE, columns), jnp.float32),
        )
        _, total, mixed = lax.fori_loop(0, (last + block - 1) // block, step, carry)
        done = (mixed / total).T.astype(jnp.bfloat16)
        for g, at in enumerate(heads):
            out[:, at] = done[g * 128 : (g + 1) * 128, :]
        return 0

    lax.fori_loop(0, 2, half, 0)


def prompt_attention(plen, q, kv, first, before):
    return pl.pallas_call(
        functools.partial(prompt_kernel, block=512),
        out_shape=jax.ShapeDtypeStruct((128, 4096), jnp.bfloat16),
        grid=(2,),
        in_specs=[
            SMEM,
            pl.BlockSpec((128, 1024), lambda i: (0, i + first)),
            pl.BlockSpec((2048, 128), lambda i: (0, i + first)),
            pl.BlockSpec((2048, 128), lambda i: (0, i + first + KEY_VALUE_HEADS)),
        ]
        + [pl.BlockSpec(memory_space=pl.ANY)] * len(before),
        out_specs=pl.BlockSpec((128, 1024), lambda i: (0, i + first)),
        input_output_aliases={4: 0} if before else {},
        compiler_params=params(24),
        cost_estimate=cost(2 * 4 * 1024 * 2048 * 128 * 3, 2 << 20, 2 * 1024 * 2048),
        name="prompt_attention",
    )(plen, q, kv, kv, *before)


def rows_kernel(*refs):
    blocks, out = refs[:-1], refs[-1]
    xh, _, y, xl, c = places()
    x = xh * 2 + xl
    for side in range(2):
        cc = c if side == 0 else 1 - c
        for part, d in enumerate(RING):
            ref = blocks[side * 4 + part]
            for n, inner in enumerate(RING):
                dx = jnp.where(cc == 0, inner, d)
                dy = jnp.where(cc == 0, d, inner)
                xx, yy = lax.rem(x + dx + 4, 4), lax.rem(y + dy + 4, 4)
                row = (xx // 2) * 512 + yy * 128 + lax.rem(xx, 2) * 64 + cc * 32
                out[pl.ds(pl.multiple_of(row, 32), 32), :] = ref[n * 32 : (n + 1) * 32, :]


def assemble_rows(blocks):
    return pl.pallas_call(
        rows_kernel,
        out_shape=jax.ShapeDtypeStruct((1024, 4096), jnp.bfloat16),
        in_specs=[VMEM] * 8,
        out_specs=VMEM,
        compiler_params=params(24),
        cost_estimate=cost(10**9, 16 << 20),
        name="assemble_rows",
    )(*blocks)


def weights_kernel(*refs):
    slices, w = refs[:-1], refs[-1]
    xh = places()[0]
    n = len(slices) // 2
    for part, half in ((slices[:n], xh), (slices[n:], 1 - xh)):
        at = half * 2048
        for ref in part:
            w[pl.ds(pl.multiple_of(at, 128), ref.shape[0]), :] = ref[...]
            at = at + ref.shape[0]


def assemble_weights(first, second):
    return pl.pallas_call(
        weights_kernel,
        out_shape=jax.ShapeDtypeStruct((4096, 896), jnp.bfloat16),
        in_specs=[VMEM] * 18,
        out_specs=VMEM,
        compiler_params=params(24),
        cost_estimate=cost(10**9, 14 << 20),
        name="assemble_weights",
    )(*first, *second)


def hidden_kernel(group, a, w, out):
    def tile(i, _):
        rows = pl.ds(pl.multiple_of(group[0] * 512 + i * 256, 256), 256)
        here = pl.ds(pl.multiple_of(i * 256, 256), 256)

        def put(lanes, gate, up):
            out[here, lanes] = (gate / (1.0 + jnp.exp(-gate)) * up).astype(jnp.bfloat16)

        def block(b, _):
            cols = pl.ds(pl.multiple_of(b * 256, 256), 256)
            both = jnp.dot(a[rows, :], w[:, cols], preferred_element_type=jnp.float32)
            put(pl.ds(pl.multiple_of(b * 128, 128), 128), both[:, :128], both[:, 128:])
            return 0

        lax.fori_loop(0, 3, block, 0)
        both = jnp.dot(a[rows, :], w[:, 768:896], preferred_element_type=jnp.float32)
        put(slice(384, 448), both[:, :64], both[:, 64:])
        return 0

    lax.fori_loop(0, 2, tile, 0)


def hidden_part(group, a, w):
    return pl.pallas_call(
        hidden_kernel,
        out_shape=jax.ShapeDtypeStruct((512, 448), jnp.bfloat16),
        in_specs=[SMEM, VMEM, VMEM],
        out_specs=VMEM,
        compiler_params=params(24),
        cost_estimate=cost(2 * 512 * 4096 * 896, 12 << 20),
        name="hidden_part",
    )(group, a, w)


def local(
    prompt_q,
    prompt_k,
    prompt_v,
    prompt_len,
    resp_q,
    resp_k,
    resp_v,
    resp_len,
    resp_resid,
    norm_gain,
    gate_weight,
    up_weight,
):
    xh = lax.axis_index("xh").astype(jnp.int32)
    own = jnp.concatenate([prompt_k[0], prompt_v[0]], axis=1)
    pair = jnp.concatenate([own, shift(own, "xl", 1)], axis=0)
    blocks = shared(ring4(pair, "y", along_y))

    mine, theirs = pack(gate_weight, up_weight)
    first = ring8(mine)
    second = ring8(shift(theirs, "xh", 1))

    kv, rows = resp_attention(
        prompt_len,
        resp_len,
        blocks,
        resp_q[0],
        resp_k[0],
        resp_v[0],
        resp_resid[0],
        norm_gain.reshape(1, -1),
    )
    axes = ("xh",) + CTX
    line = jnp.concatenate(ring4(rows, axes, functools.partial(crossed, True)), axis=0)
    plane = ring4(line, axes, functools.partial(crossed, False))
    blocks = shared(plane)
    first[4] = farthest(first, line)
    out = prompt_attention(prompt_len, prompt_q[0], kv, 0, ())

    second[4] = farthest(second, plane[1])
    rows = assemble_rows(blocks)
    w = assemble_weights(*([a for d in NEAR + FAR for a in s[d]] for s in (first, second)))
    away = hidden_part((1 - xh).reshape(1), rows, w)
    got = shift(away, "xh", 1)
    done = hidden_part(xh.reshape(1), rows, w)
    out = prompt_attention(prompt_len, prompt_q[0], kv, 2, (out,))
    zero = jnp.where(xh == 0, done, got)
    one = jnp.where(xh == 0, got, done)
    hidden = jnp.concatenate([zero, one[:, 384:], one[:, :384]], axis=1)
    return (out[None], hidden[None])


def solution(mesh):
    finer = Mesh(mesh.devices.reshape(2, 8, 4, 2, 2), ("xh", "z", "y", "xl", "c"))

    return jax.shard_map(
        local,
        mesh=finer,
        in_specs=(
            P(DP, CTX, None),
            P(DP, CTX, None),
            P(DP, CTX, None),
            P(DP),
            P(DP, CTX, None),
            P(DP, CTX, None),
            P(DP, CTX, None),
            P(DP, CTX),
            P(DP, CTX, None),
            P(),
            P(DP, CTX),
            P(DP, CTX),
        ),
        out_specs=(P(DP, CTX, None), P(DP, None, CTX)),
        check_vma=False,
    )
```

```python
import functools

import jax
import jax.numpy as jnp
from jax import lax
from jax.experimental import pallas as pl
from jax.experimental.pallas import tpu as pltpu
from jax.sharding import Mesh
from jax.sharding import PartitionSpec as P

KEY_VALUE_HEADS = 4
GROUP = 8
HEAD_SIZE = 128
RLEN = 16
CTX = ("y", "xl", "c")
DP = ("xh", "z")
TO_LOG2 = 1.4426950408889634 * HEAD_SIZE**-0.5
HIDDEN = -1e30
VMEM = pl.BlockSpec(memory_space=pltpu.VMEM)
SMEM = pl.BlockSpec(memory_space=pltpu.SMEM)


def params(limit):
    return pltpu.CompilerParams(vmem_limit_bytes=limit << 20)


def cost(flops, moved, exps=0):
    return pl.CostEstimate(flops=flops, bytes_accessed=moved, transcendentals=exps)


def shift(a, axis, by):
    n = lax.axis_size(axis)
    return lax.ppermute(a, axis, [(i, (i + by) % n) for i in range(n)])


def halves(a, axis):
    n = a.shape[axis] // 2
    return lax.slice_in_dim(a, 0, n, axis=axis), lax.slice_in_dim(a, n, 2 * n, axis=axis)


def ring4(a, axes, pairs):
    low = lax.ppermute(a, axes, pairs(1))
    high = lax.ppermute(a, axes, pairs(-1))
    far_a = lax.ppermute(halves(low, 0)[0], axes, pairs(1))
    far_b = lax.ppermute(halves(high, 0)[1], axes, pairs(-1))
    return [a, low, high, jnp.concatenate([far_a, far_b], axis=0)]


def shared(pieces):
    return pieces + [shift(a, "c", 1) for a in pieces]


def along_y(by):
    return [(i, (i + by) % 4) for i in range(4)]


def crossed(x_first, by):
    def flat(x, y, c):
        return ((x // 2 * 4 + y) * 2 + x % 2) * 2 + c

    out = []
    for x in range(4):
        for y in range(4):
            for c in range(2):
                to = ((x + by) % 4, y) if (c == 0) == x_first else (x, (y + by) % 4)
                out.append((flat(x, y, c), flat(*to, c)))
    return out


RING = (0, -1, 1, 2)


def places():
    return [lax.axis_index(a).astype(jnp.int32) for a in ("xh", "z", "y", "xl", "c")]


def pack_kernel(gate, up, mine, theirs):
    xh = places()[0]

    def pack(half, out):
        start, tail = (0, 384) if half == 0 else (512, 448)
        for b in range(3):
            at = start + 128 * b
            out[:, 256 * b : 256 * b + 128] = gate[:, at : at + 128]
            out[:, 256 * b + 128 : 256 * b + 256] = up[:, at : at + 128]
        out[:, 768:832] = gate[:, tail : tail + 64]
        out[:, 832:896] = up[:, tail : tail + 64]

    @pl.when(xh == 0)
    def _():
        pack(0, mine)
        pack(1, theirs)

    @pl.when(xh != 0)
    def _():
        pack(1, mine)
        pack(0, theirs)


def pack(gate, up):
    shape = jax.ShapeDtypeStruct(gate.shape, gate.dtype)
    return pl.pallas_call(
        pack_kernel,
        out_shape=(shape, shape),
        in_specs=[VMEM, VMEM],
        out_specs=(VMEM, VMEM),
        compiler_params=params(8),
        cost_estimate=cost(10**9, 2 * 2 * gate.size * 2),
        name="pack",
    )(gate, up)


def ring8(shard):
    pairs = []
    for z in range(8):
        for c in range(2):
            pairs.append((z * 2 + c, (z + (1, -1)[c]) % 8 * 2 + c))
    pieces = [shard]
    for _ in range(1, 8):
        pieces.append(lax.ppermute(pieces[-1], ("z", "c"), pairs))
    return pieces


ROWS = (((1,), (1,)), ((), ()))


def resp_kernel(plen, rlen, *refs):
    blocks, (q, rk, rv, resid, gain, kv, out, attn) = refs[:6], refs[6:]
    _, _, y, xl, c = places()
    limit, len0, len1 = plen[0], rlen[0, 0], rlen[0, 1]
    for i in range(8):
        cc = c if i < 4 else 1 - c
        ref, at = (blocks[i], 0) if i < 4 else (blocks[4], (i - 4) * 256) if i < 7 else (blocks[5], 0)
        yy = lax.rem(y + RING[i % 4] + 4, 4)
        for beside in range(2):
            xx = xl if beside == 0 else 1 - xl
            row = pl.multiple_of(((yy * 2 + xx) * 2 + cc) * 128, 128)
            kv[pl.ds(row, 128), :] = ref[at + beside * 128 : at + (beside + 1) * 128, :]
    rows = GROUP * 32
    r = lax.rem(lax.broadcasted_iota(jnp.int32, (rows, 32), 0), 32)
    t = lax.broadcasted_iota(jnp.int32, (rows, 32), 1)
    slot_t, place_t = t // RLEN, lax.rem(t, RLEN)
    own = (
        (r // RLEN == slot_t)
        & (place_t <= lax.rem(r, RLEN))
        & (place_t < jnp.where(slot_t == 0, len0, len1))
    )
    column = lax.broadcasted_iota(jnp.int32, (rows, 2048), 1)

    def head(h, _):
        lanes = pl.ds(pl.multiple_of(h * HEAD_SIZE, HEAD_SIZE), HEAD_SIZE)
        behind = pl.ds(pl.multiple_of(512 + h * HEAD_SIZE, HEAD_SIZE), HEAD_SIZE)
        heads = [
            pl.ds(pl.multiple_of((h * GROUP + g) * HEAD_SIZE, HEAD_SIZE), HEAD_SIZE) for g in range(GROUP)
        ]
        qs = jnp.concatenate([q[:, at] for at in heads], axis=0)
        s_own = lax.dot_general(qs, rk[:, lanes], ROWS, preferred_element_type=jnp.float32)
        s_own = jnp.where(own, s_own, HIDDEN)
        s = lax.dot_general(qs, kv[:, lanes], ROWS, preferred_element_type=jnp.float32)
        s = jnp.where(column < limit, s, HIDDEN)
        top = jnp.maximum(jnp.max(s, axis=1, keepdims=True), jnp.max(s_own, axis=1, keepdims=True))
        w = jnp.exp2((s - top) * TO_LOG2)
        w_own = jnp.exp2((s_own - top) * TO_LOG2)
        total = jnp.sum(w, axis=1, keepdims=True) + jnp.sum(w_own, axis=1, keepdims=True)
        mixed = jnp.dot(w.astype(jnp.bfloat16), kv[:, behind], preferred_element_type=jnp.float32)
        mixed += jnp.dot(w_own.astype(jnp.bfloat16), rv[:, lanes], preferred_element_type=jnp.float32)
        done = (mixed / total).astype(jnp.bfloat16)
        for g, at in enumerate(heads):
            attn[:, at] = done[g * 32 : (g + 1) * 32, :]
        return 0

    lax.fori_loop(0, KEY_VALUE_HEADS, head, 0)
    stream = resid[...].astype(jnp.float32) + attn[...].astype(jnp.float32)
    scale = lax.rsqrt(jnp.mean(stream * stream, axis=1, keepdims=True) + 1e-05)
    out[...] = (stream * scale * gain[...]).astype(jnp.bfloat16)


def resp_attention(plen, rlen, blocks, q, rk, rv, resid, gain):
    return pl.pallas_call(
        resp_kernel,
        out_shape=(
            jax.ShapeDtypeStruct((2048, 1024), jnp.bfloat16),
            jax.ShapeDtypeStruct((32, 4096), jnp.bfloat16),
        ),
        in_specs=[SMEM, SMEM] + [VMEM] * 11,
        out_specs=(VMEM, VMEM),
        scratch_shapes=[pltpu.VMEM((32, 4096), jnp.bfloat16)],
        compiler_params=params(20),
        cost_estimate=cost(4 * 1024 * 2080 * 128, 9 << 20, 1024 * 2080),
        name="resp_attention",
    )(plen, rlen, *blocks, q, rk, rv, resid, gain)


def prompt_kernel(plen, q, keys, values, *refs):
    out = refs[-1]
    _, _, y, xl, c = places()
    here = (y * 2 + xl) * 2 + c
    rows = 2 * 128
    place = lax.rem(lax.broadcasted_iota(jnp.int32, (rows, 1), 0), 128)
    ends = jnp.minimum(here * 128 + place + 1, plen[0])
    column = lax.broadcasted_iota(jnp.int32, (rows, 2048), 1)

    def two_heads(i, _):
        heads = [pl.ds(pl.multiple_of((i * 2 + g) * HEAD_SIZE, HEAD_SIZE), HEAD_SIZE) for g in range(2)]
        qs = jnp.concatenate([q[:, at] for at in heads], axis=0)
        s = lax.dot_general(qs, keys[...], ROWS, preferred_element_type=jnp.float32)
        s = jnp.where(column < ends, s, HIDDEN)
        top = jnp.max(s, axis=1, keepdims=True)
        w = jnp.exp2((s - top) * TO_LOG2)
        total = jnp.sum(w, axis=1, keepdims=True)
        mixed = jnp.dot(w.astype(jnp.bfloat16), values[...], preferred_element_type=jnp.float32)
        done = (mixed / total).astype(jnp.bfloat16)
        for g, at in enumerate(heads):
            out[:, at] = done[g * 128 : (g + 1) * 128, :]
        return 0

    lax.fori_loop(0, GROUP // 2, two_heads, 0)


def prompt_attention(plen, q, kv, first, before):
    return pl.pallas_call(
        prompt_kernel,
        out_shape=jax.ShapeDtypeStruct((128, 4096), jnp.bfloat16),
        grid=(2,),
        in_specs=[
            SMEM,
            pl.BlockSpec((128, 1024), lambda i: (0, i + first)),
            pl.BlockSpec((2048, 128), lambda i: (0, i + first)),
            pl.BlockSpec((2048, 128), lambda i: (0, i + first + KEY_VALUE_HEADS)),
        ]
        + [pl.BlockSpec(memory_space=pl.ANY)] * len(before),
        out_specs=pl.BlockSpec((128, 1024), lambda i: (0, i + first)),
        input_output_aliases={4: 0} if before else {},
        compiler_params=params(16),
        cost_estimate=cost(2 * 4 * 1024 * 2048 * 128 * 3, 2 << 20, 2 * 1024 * 2048),
        name="prompt_attention",
    )(plen, q, kv, kv, *before)


def rows_kernel(*refs):
    blocks, out = refs[:-1], refs[-1]
    xh, _, y, xl, c = places()
    x = xh * 2 + xl
    for side in range(2):
        cc = c if side == 0 else 1 - c
        for part, d in enumerate(RING):
            ref = blocks[side * 4 + part]
            for n, inner in enumerate(RING):
                dx = jnp.where(cc == 0, inner, d)
                dy = jnp.where(cc == 0, d, inner)
                xx, yy = lax.rem(x + dx + 4, 4), lax.rem(y + dy + 4, 4)
                row = (xx // 2) * 512 + yy * 128 + lax.rem(xx, 2) * 64 + cc * 32
                out[pl.ds(pl.multiple_of(row, 32), 32), :] = ref[n * 32 : (n + 1) * 32, :]


def assemble_rows(blocks):
    return pl.pallas_call(
        rows_kernel,
        out_shape=jax.ShapeDtypeStruct((1024, 4096), jnp.bfloat16),
        in_specs=[VMEM] * 8,
        out_specs=VMEM,
        compiler_params=params(24),
        cost_estimate=cost(10**9, 16 << 20),
        name="assemble_rows",
    )(*blocks)


def weights_kernel(*refs):
    slices, w = refs[:-1], refs[-1]
    xh, z, _, _, c = places()
    for i, ref in enumerate(slices):
        half = xh if i < 8 else 1 - xh
        from_z = lax.rem(z + jnp.where(c == 0, 8 - i % 8, i % 8), 8)
        w[pl.ds(pl.multiple_of((half * 8 + from_z) * 256, 256), 256), :] = ref[...]


def assemble_weights(slices):
    return pl.pallas_call(
        weights_kernel,
        out_shape=jax.ShapeDtypeStruct((4096, 896), jnp.bfloat16),
        in_specs=[VMEM] * 16,
        out_specs=VMEM,
        compiler_params=params(20),
        cost_estimate=cost(10**9, 14 << 20),
        name="assemble_weights",
    )(*slices)


def hidden_kernel(group, a, w, out):
    def tile(i, _):
        rows = pl.ds(pl.multiple_of(group[0] * 512 + i * 256, 256), 256)
        here = pl.ds(pl.multiple_of(i * 256, 256), 256)

        def put(lanes, gate, up):
            out[here, lanes] = (gate / (1.0 + jnp.exp(-gate)) * up).astype(jnp.bfloat16)

        def block(b, _):
            cols = pl.ds(pl.multiple_of(b * 256, 256), 256)
            both = jnp.dot(a[rows, :], w[:, cols], preferred_element_type=jnp.float32)
            put(pl.ds(pl.multiple_of(b * 128, 128), 128), both[:, :128], both[:, 128:])
            return 0

        lax.fori_loop(0, 3, block, 0)
        both = jnp.dot(a[rows, :], w[:, 768:896], preferred_element_type=jnp.float32)
        put(slice(384, 448), both[:, :64], both[:, 64:])
        return 0

    lax.fori_loop(0, 2, tile, 0)


def hidden_part(group, a, w):
    return pl.pallas_call(
        hidden_kernel,
        out_shape=jax.ShapeDtypeStruct((512, 448), jnp.bfloat16),
        in_specs=[SMEM, VMEM, VMEM],
        out_specs=VMEM,
        compiler_params=params(24),
        cost_estimate=cost(2 * 512 * 4096 * 896, 12 << 20),
        name="hidden_part",
    )(group, a, w)


def local(
    prompt_q,
    prompt_k,
    prompt_v,
    prompt_len,
    resp_q,
    resp_k,
    resp_v,
    resp_len,
    resp_resid,
    norm_gain,
    gate_weight,
    up_weight,
):
    xh = lax.axis_index("xh").astype(jnp.int32)
    own = jnp.concatenate([prompt_k[0], prompt_v[0]], axis=1)
    pair = jnp.concatenate([own, shift(own, "xl", 1)], axis=0)
    blocks = ring4(pair, "y", along_y)
    blocks = blocks + [shift(jnp.concatenate(blocks[:3], axis=0), "c", 1), shift(blocks[3], "c", 1)]

    mine, theirs = pack(gate_weight, up_weight)
    first = ring8(mine)
    second = ring8(shift(theirs, "xh", 1))

    kv, rows = resp_attention(
        prompt_len,
        resp_len,
        blocks,
        resp_q[0],
        resp_k[0],
        resp_v[0],
        resp_resid[0],
        norm_gain.reshape(1, -1),
    )
    axes = ("xh",) + CTX
    line = jnp.concatenate(ring4(rows, axes, functools.partial(crossed, True)), axis=0)
    plane = ring4(line, axes, functools.partial(crossed, False))
    blocks = shared(plane)
    out = prompt_attention(prompt_len, prompt_q[0], kv, 0, ())

    rows = assemble_rows(blocks)
    w = assemble_weights(first + second)
    away = hidden_part((1 - xh).reshape(1), rows, w)
    got = shift(away, "xh", 1)
    done = hidden_part(xh.reshape(1), rows, w)
    out = prompt_attention(prompt_len, prompt_q[0], kv, 2, (out,))
    zero = jnp.where(xh == 0, done, got)
    one = jnp.where(xh == 0, got, done)
    hidden = jnp.concatenate([zero, one[:, 384:], one[:, :384]], axis=1)
    return (out[None], hidden[None])


def solution(mesh):
    finer = Mesh(mesh.devices.reshape(2, 8, 4, 2, 2), ("xh", "z", "y", "xl", "c"))

    return jax.shard_map(
        local,
        mesh=finer,
        in_specs=(
            P(DP, CTX, None),
            P(DP, CTX, None),
            P(DP, CTX, None),
            P(DP),
            P(DP, CTX, None),
            P(DP, CTX, None),
            P(DP, CTX, None),
            P(DP, CTX),
            P(DP, CTX, None),
            P(),
            P(DP, CTX),
            P(DP, CTX),
        ),
        out_specs=(P(DP, CTX, None), P(DP, None, CTX)),
        check_vma=False,
    )
```

```python
import functools

import jax
import jax.numpy as jnp
from jax import lax
from jax.experimental import pallas as pl
from jax.experimental.pallas import tpu as pltpu
from jax.sharding import Mesh
from jax.sharding import PartitionSpec as P

KEY_VALUE_HEADS = 4
GROUP = 8
HEAD_SIZE = 128
RLEN = 16
CTX = ("y", "xl", "c")
DP = ("xh", "z")
TO_LOG2 = 1.4426950408889634 * HEAD_SIZE**-0.5
HIDDEN = -1e30
VMEM = pl.BlockSpec(memory_space=pltpu.VMEM)
SMEM = pl.BlockSpec(memory_space=pltpu.SMEM)


def params(limit):
    return pltpu.CompilerParams(vmem_limit_bytes=limit << 20)


def cost(flops, moved, exps=0):
    return pl.CostEstimate(flops=flops, bytes_accessed=moved, transcendentals=exps)


def shift(a, axis, by):
    n = lax.axis_size(axis)
    return lax.ppermute(a, axis, [(i, (i + by) % n) for i in range(n)])


def ring4(a, axes, pairs):
    return [a] + [lax.ppermute(a, axes, pairs(by)) for by in (1, -1, 2)]


def shared(pieces):
    return pieces + [shift(a, "c", 1) for a in pieces]


def along_y(by):
    return [(i, (i + by) % 4) for i in range(4)]


def crossed(x_first, by):
    def flat(x, y, c):
        return ((x // 2 * 4 + y) * 2 + x % 2) * 2 + c

    out = []
    for x in range(4):
        for y in range(4):
            for c in range(2):
                to = ((x + by) % 4, y) if (c == 0) == x_first else (x, (y + by) % 4)
                out.append((flat(x, y, c), flat(*to, c)))
    return out


RING = (0, -1, 1, 2)


def places():
    return [lax.axis_index(a).astype(jnp.int32) for a in ("xh", "z", "y", "xl", "c")]


def pack_kernel(gate, up, mine, theirs):
    xh = places()[0]

    def pack(half, out):
        start, tail = (0, 384) if half == 0 else (512, 448)
        for b in range(3):
            at = start + 128 * b
            out[:, 256 * b : 256 * b + 128] = gate[:, at : at + 128]
            out[:, 256 * b + 128 : 256 * b + 256] = up[:, at : at + 128]
        out[:, 768:832] = gate[:, tail : tail + 64]
        out[:, 832:896] = up[:, tail : tail + 64]

    @pl.when(xh == 0)
    def _():
        pack(0, mine)
        pack(1, theirs)

    @pl.when(xh != 0)
    def _():
        pack(1, mine)
        pack(0, theirs)


def pack(gate, up):
    shape = jax.ShapeDtypeStruct(gate.shape, gate.dtype)
    return pl.pallas_call(
        pack_kernel,
        out_shape=(shape, shape),
        in_specs=[VMEM, VMEM],
        out_specs=(VMEM, VMEM),
        compiler_params=params(8),
        cost_estimate=cost(10**9, 2 * 2 * gate.size * 2),
        name="pack",
    )(gate, up)


def ring8(shard):
    pairs = []
    for z in range(8):
        for c in range(2):
            pairs.append((z * 2 + c, (z + (1, -1)[c]) % 8 * 2 + c))
    pieces = [shard]
    for _ in range(1, 8):
        pieces.append(lax.ppermute(pieces[-1], ("z", "c"), pairs))
    return pieces


ROWS = (((1,), (1,)), ((), ()))


def resp_kernel(plen, rlen, *refs):
    blocks, (q, rk, rv, resid, gain, kv, out, attn) = refs[:6], refs[6:]
    _, _, y, xl, c = places()
    limit, len0, len1 = plen[0], rlen[0, 0], rlen[0, 1]
    for i in range(8):
        cc = c if i < 4 else 1 - c
        ref, at = (blocks[i], 0) if i < 4 else (blocks[4], (i - 4) * 256) if i < 7 else (blocks[5], 0)
        yy = lax.rem(y + RING[i % 4] + 4, 4)
        for beside in range(2):
            xx = xl if beside == 0 else 1 - xl
            row = pl.multiple_of(((yy * 2 + xx) * 2 + cc) * 128, 128)
            kv[pl.ds(row, 128), :] = ref[at + beside * 128 : at + (beside + 1) * 128, :]
    rows = GROUP * 32
    r = lax.rem(lax.broadcasted_iota(jnp.int32, (rows, 32), 0), 32)
    t = lax.broadcasted_iota(jnp.int32, (rows, 32), 1)
    slot_t, place_t = t // RLEN, lax.rem(t, RLEN)
    own = (
        (r // RLEN == slot_t)
        & (place_t <= lax.rem(r, RLEN))
        & (place_t < jnp.where(slot_t == 0, len0, len1))
    )
    column = lax.broadcasted_iota(jnp.int32, (rows, 2048), 1)

    def head(h, _):
        lanes = pl.ds(pl.multiple_of(h * HEAD_SIZE, HEAD_SIZE), HEAD_SIZE)
        behind = pl.ds(pl.multiple_of(512 + h * HEAD_SIZE, HEAD_SIZE), HEAD_SIZE)
        heads = [
            pl.ds(pl.multiple_of((h * GROUP + g) * HEAD_SIZE, HEAD_SIZE), HEAD_SIZE) for g in range(GROUP)
        ]
        qs = jnp.concatenate([q[:, at] for at in heads], axis=0)
        s_own = lax.dot_general(qs, rk[:, lanes], ROWS, preferred_element_type=jnp.float32)
        s_own = jnp.where(own, s_own, HIDDEN)
        s = lax.dot_general(qs, kv[:, lanes], ROWS, preferred_element_type=jnp.float32)
        s = jnp.where(column < limit, s, HIDDEN)
        top = jnp.maximum(jnp.max(s, axis=1, keepdims=True), jnp.max(s_own, axis=1, keepdims=True))
        w = jnp.exp2((s - top) * TO_LOG2)
        w_own = jnp.exp2((s_own - top) * TO_LOG2)
        total = jnp.sum(w, axis=1, keepdims=True) + jnp.sum(w_own, axis=1, keepdims=True)
        mixed = jnp.dot(w.astype(jnp.bfloat16), kv[:, behind], preferred_element_type=jnp.float32)
        mixed += jnp.dot(w_own.astype(jnp.bfloat16), rv[:, lanes], preferred_element_type=jnp.float32)
        done = (mixed / total).astype(jnp.bfloat16)
        for g, at in enumerate(heads):
            attn[:, at] = done[g * 32 : (g + 1) * 32, :]
        return 0

    lax.fori_loop(0, KEY_VALUE_HEADS, head, 0)
    stream = resid[...].astype(jnp.float32) + attn[...].astype(jnp.float32)
    scale = lax.rsqrt(jnp.mean(stream * stream, axis=1, keepdims=True) + 1e-05)
    out[...] = (stream * scale * gain[...]).astype(jnp.bfloat16)


def resp_attention(plen, rlen, blocks, q, rk, rv, resid, gain):
    return pl.pallas_call(
        resp_kernel,
        out_shape=(
            jax.ShapeDtypeStruct((2048, 1024), jnp.bfloat16),
            jax.ShapeDtypeStruct((32, 4096), jnp.bfloat16),
        ),
        in_specs=[SMEM, SMEM] + [VMEM] * 11,
        out_specs=(VMEM, VMEM),
        scratch_shapes=[pltpu.VMEM((32, 4096), jnp.bfloat16)],
        compiler_params=params(20),
        cost_estimate=cost(4 * 1024 * 2080 * 128, 9 << 20, 1024 * 2080),
        name="resp_attention",
    )(plen, rlen, *blocks, q, rk, rv, resid, gain)


def prompt_kernel(plen, q, keys, values, *refs):
    out = refs[-1]
    _, _, y, xl, c = places()
    here = (y * 2 + xl) * 2 + c
    rows = 2 * 128
    place = lax.rem(lax.broadcasted_iota(jnp.int32, (rows, 1), 0), 128)
    ends = jnp.minimum(here * 128 + place + 1, plen[0])
    column = lax.broadcasted_iota(jnp.int32, (rows, 2048), 1)

    def two_heads(i, _):
        heads = [pl.ds(pl.multiple_of((i * 2 + g) * HEAD_SIZE, HEAD_SIZE), HEAD_SIZE) for g in range(2)]
        qs = jnp.concatenate([q[:, at] for at in heads], axis=0)
        s = lax.dot_general(qs, keys[...], ROWS, preferred_element_type=jnp.float32)
        s = jnp.where(column < ends, s, HIDDEN)
        top = jnp.max(s, axis=1, keepdims=True)
        w = jnp.exp2((s - top) * TO_LOG2)
        total = jnp.sum(w, axis=1, keepdims=True)
        mixed = jnp.dot(w.astype(jnp.bfloat16), values[...], preferred_element_type=jnp.float32)
        done = (mixed / total).astype(jnp.bfloat16)
        for g, at in enumerate(heads):
            out[:, at] = done[g * 128 : (g + 1) * 128, :]
        return 0

    lax.fori_loop(0, GROUP // 2, two_heads, 0)


def prompt_attention(plen, q, kv, first, count, before):
    return pl.pallas_call(
        prompt_kernel,
        out_shape=jax.ShapeDtypeStruct((128, 4096), jnp.bfloat16),
        grid=(count,),
        in_specs=[
            SMEM,
            pl.BlockSpec((128, 1024), lambda i: (0, i + first)),
            pl.BlockSpec((2048, 128), lambda i: (0, i + first)),
            pl.BlockSpec((2048, 128), lambda i: (0, i + first + KEY_VALUE_HEADS)),
        ]
        + [pl.BlockSpec(memory_space=pl.ANY)] * len(before),
        out_specs=pl.BlockSpec((128, 1024), lambda i: (0, i + first)),
        input_output_aliases={4: 0} if before else {},
        compiler_params=params(16),
        cost_estimate=cost(count * 12 * 1024 * 2048 * 128, count << 20, count * 1024 * 2048),
        name="prompt_attention",
    )(plen, q, kv, kv, *before)


def rows_kernel(*refs):
    blocks, out = refs[:-1], refs[-1]
    xh, _, y, xl, c = places()
    x = xh * 2 + xl
    for side in range(2):
        cc = c if side == 0 else 1 - c
        for part, d in enumerate(RING):
            ref = blocks[side * 4 + part]
            for n, inner in enumerate(RING):
                dx = jnp.where(cc == 0, inner, d)
                dy = jnp.where(cc == 0, d, inner)
                xx, yy = lax.rem(x + dx + 4, 4), lax.rem(y + dy + 4, 4)
                row = (xx // 2) * 512 + yy * 128 + lax.rem(xx, 2) * 64 + cc * 32
                out[pl.ds(pl.multiple_of(row, 32), 32), :] = ref[n * 32 : (n + 1) * 32, :]


def assemble_rows(blocks):
    return pl.pallas_call(
        rows_kernel,
        out_shape=jax.ShapeDtypeStruct((1024, 4096), jnp.bfloat16),
        in_specs=[VMEM] * 8,
        out_specs=VMEM,
        compiler_params=params(24),
        cost_estimate=cost(10**9, 16 << 20),
        name="assemble_rows",
    )(*blocks)


def weights_kernel(*refs):
    slices, w = refs[:-1], refs[-1]
    xh, z, _, _, c = places()
    for i, ref in enumerate(slices):
        half = xh if i < 8 else 1 - xh
        from_z = lax.rem(z + jnp.where(c == 0, 8 - i % 8, i % 8), 8)
        w[pl.ds(pl.multiple_of((half * 8 + from_z) * 256, 256), 256), :] = ref[...]


def assemble_weights(slices):
    return pl.pallas_call(
        weights_kernel,
        out_shape=jax.ShapeDtypeStruct((4096, 896), jnp.bfloat16),
        in_specs=[VMEM] * 16,
        out_specs=VMEM,
        compiler_params=params(20),
        cost_estimate=cost(10**9, 14 << 20),
        name="assemble_weights",
    )(*slices)


def hidden_kernel(group, a, w, out):
    rows = pl.ds(pl.multiple_of(group[0] * 512, 512), 512)

    def put(lanes, gate, up):
        out[:, lanes] = (gate / (1.0 + jnp.exp(-gate)) * up).astype(jnp.bfloat16)

    def block(b, _):
        cols = pl.ds(pl.multiple_of(b * 256, 256), 256)
        both = jnp.dot(a[rows, :], w[:, cols], preferred_element_type=jnp.float32)
        put(pl.ds(pl.multiple_of(b * 128, 128), 128), both[:, :128], both[:, 128:])
        return 0

    lax.fori_loop(0, 3, block, 0)
    both = jnp.dot(a[rows, :], w[:, 768:896], preferred_element_type=jnp.float32)
    put(slice(384, 448), both[:, :64], both[:, 64:])


def hidden_part(group, a, w):
    return pl.pallas_call(
        hidden_kernel,
        out_shape=jax.ShapeDtypeStruct((512, 448), jnp.bfloat16),
        in_specs=[SMEM, VMEM, VMEM],
        out_specs=VMEM,
        compiler_params=params(24),
        cost_estimate=cost(2 * 512 * 4096 * 896, 12 << 20),
        name="hidden_part",
    )(group, a, w)


def local(
    prompt_q,
    prompt_k,
    prompt_v,
    prompt_len,
    resp_q,
    resp_k,
    resp_v,
    resp_len,
    resp_resid,
    norm_gain,
    gate_weight,
    up_weight,
):
    xh = lax.axis_index("xh").astype(jnp.int32)
    own = jnp.concatenate([prompt_k[0], prompt_v[0]], axis=1)
    pair = jnp.concatenate([own, shift(own, "xl", 1)], axis=0)
    blocks = ring4(pair, "y", along_y)
    blocks = blocks + [shift(jnp.concatenate(blocks[:3], axis=0), "c", 1), shift(blocks[3], "c", 1)]

    mine, theirs = pack(gate_weight, up_weight)
    first = ring8(mine)
    second = ring8(shift(theirs, "xh", 1))

    kv, rows = resp_attention(
        prompt_len,
        resp_len,
        blocks,
        resp_q[0],
        resp_k[0],
        resp_v[0],
        resp_resid[0],
        norm_gain.reshape(1, -1),
    )
    axes = ("xh",) + CTX
    line = jnp.concatenate(ring4(rows, axes, functools.partial(crossed, True)), axis=0)
    plane = ring4(line, axes, functools.partial(crossed, False))
    blocks = shared(plane)
    out = prompt_attention(prompt_len, prompt_q[0], kv, 0, 2, ())

    out = prompt_attention(prompt_len, prompt_q[0], kv, 2, 1, (out,))

    rows = assemble_rows(blocks)
    w = assemble_weights(first + second)
    away = hidden_part((1 - xh).reshape(1), rows, w)
    got = shift(away, "xh", 1)
    done = hidden_part(xh.reshape(1), rows, w)
    out = prompt_attention(prompt_len, prompt_q[0], kv, 3, 1, (out,))
    zero = jnp.where(xh == 0, done, got)
    one = jnp.where(xh == 0, got, done)
    hidden = jnp.concatenate([zero, one[:, 384:], one[:, :384]], axis=1)
    return (out[None], hidden[None])


def solution(mesh):
    finer = Mesh(mesh.devices.reshape(2, 8, 4, 2, 2), ("xh", "z", "y", "xl", "c"))

    return jax.shard_map(
        local,
        mesh=finer,
        in_specs=(
            P(DP, CTX, None),
            P(DP, CTX, None),
            P(DP, CTX, None),
            P(DP),
            P(DP, CTX, None),
            P(DP, CTX, None),
            P(DP, CTX, None),
            P(DP, CTX),
            P(DP, CTX, None),
            P(),
            P(DP, CTX),
            P(DP, CTX),
        ),
        out_specs=(P(DP, CTX, None), P(DP, None, CTX)),
        check_vma=False,
    )
```

```python
import functools

import jax
import jax.numpy as jnp
from jax import lax
from jax.experimental import pallas as pl
from jax.experimental.pallas import tpu as pltpu
from jax.sharding import Mesh
from jax.sharding import PartitionSpec as P

KEY_VALUE_HEADS = 4
GROUP = 8
HEAD_SIZE = 128
RLEN = 16
CTX = ("y", "xl", "c")
DP = ("xh", "z")
TO_LOG2 = 1.4426950408889634 * HEAD_SIZE**-0.5
HIDDEN = -1e30
VMEM = pl.BlockSpec(memory_space=pltpu.VMEM)
SMEM = pl.BlockSpec(memory_space=pltpu.SMEM)


def params(limit):
    return pltpu.CompilerParams(vmem_limit_bytes=limit << 20)


def cost(flops, moved, exps=0):
    return pl.CostEstimate(flops=flops, bytes_accessed=moved, transcendentals=exps)


def shift(a, axis, by):
    n = lax.axis_size(axis)
    return lax.ppermute(a, axis, [(i, (i + by) % n) for i in range(n)])


def halves(a, axis):
    n = a.shape[axis] // 2
    return lax.slice_in_dim(a, 0, n, axis=axis), lax.slice_in_dim(a, n, 2 * n, axis=axis)


def ring4(a, axes, pairs):
    return [a] + [lax.ppermute(a, axes, pairs(by)) for by in (1, -1, 2)]


def ring4_halves(a, axes, pairs):
    low = lax.ppermute(a, axes, pairs(1))
    high = lax.ppermute(a, axes, pairs(-1))
    far_a = lax.ppermute(halves(low, 0)[0], axes, pairs(1))
    far_b = lax.ppermute(halves(high, 0)[1], axes, pairs(-1))
    return [a, low, high, jnp.concatenate([far_a, far_b], axis=0)]


def shared(pieces):
    return pieces + [shift(a, "c", 1) for a in pieces]


def along_y(by):
    return [(i, (i + by) % 4) for i in range(4)]


def crossed(x_first, by):
    def flat(x, y, c):
        return ((x // 2 * 4 + y) * 2 + x % 2) * 2 + c

    out = []
    for x in range(4):
        for y in range(4):
            for c in range(2):
                to = ((x + by) % 4, y) if (c == 0) == x_first else (x, (y + by) % 4)
                out.append((flat(x, y, c), flat(*to, c)))
    return out


RING = (0, -1, 1, 2)


def places():
    return [lax.axis_index(a).astype(jnp.int32) for a in ("xh", "z", "y", "xl", "c")]


def pack_kernel(gate, up, mine, theirs):
    xh = places()[0]

    def pack(half, out):
        start, tail = (0, 384) if half == 0 else (512, 448)
        for b in range(3):
            at = start + 128 * b
            out[:, 256 * b : 256 * b + 128] = gate[:, at : at + 128]
            out[:, 256 * b + 128 : 256 * b + 256] = up[:, at : at + 128]
        out[:, 768:832] = gate[:, tail : tail + 64]
        out[:, 832:896] = up[:, tail : tail + 64]

    @pl.when(xh == 0)
    def _():
        pack(0, mine)
        pack(1, theirs)

    @pl.when(xh != 0)
    def _():
        pack(1, mine)
        pack(0, theirs)


def pack(gate, up):
    shape = jax.ShapeDtypeStruct(gate.shape, gate.dtype)
    return pl.pallas_call(
        pack_kernel,
        out_shape=(shape, shape),
        in_specs=[VMEM, VMEM],
        out_specs=(VMEM, VMEM),
        compiler_params=params(8),
        cost_estimate=cost(10**9, 2 * 2 * gate.size * 2),
        name="pack",
    )(gate, up)


def up_or_down(a):
    pairs = []
    for z in range(8):
        for c in range(2):
            pairs.append((z * 2 + c, (z + (1, -1)[c]) % 8 * 2 + c))
    return lax.ppermute(a, ("z", "c"), pairs)


def gather_slices(mine, theirs):
    second = shift(theirs, "xh", 1)
    first = up_or_down(mine)
    both = jnp.concatenate([first, second], axis=0)
    steps = []
    for _ in range(1, 7):
        both = up_or_down(both)
        steps.append(both)
    return [mine, first, second, *steps, up_or_down(halves(both, 0)[1])]


ROWS = (((1,), (1,)), ((), ()))


def resp_kernel(plen, rlen, *refs):
    blocks, (q, rk, rv, resid, gain, kv, out, attn) = refs[:6], refs[6:]
    _, _, y, xl, c = places()
    limit, len0, len1 = plen[0], rlen[0, 0], rlen[0, 1]
    for i in range(8):
        cc = c if i < 4 else 1 - c
        ref, at = (blocks[i], 0) if i < 4 else (blocks[4], (i - 4) * 256) if i < 7 else (blocks[5], 0)
        yy = lax.rem(y + RING[i % 4] + 4, 4)
        for beside in range(2):
            xx = xl if beside == 0 else 1 - xl
            row = pl.multiple_of(((yy * 2 + xx) * 2 + cc) * 128, 128)
            kv[pl.ds(row, 128), :] = ref[at + beside * 128 : at + (beside + 1) * 128, :]
    rows = GROUP * 32
    r = lax.rem(lax.broadcasted_iota(jnp.int32, (rows, 32), 0), 32)
    t = lax.broadcasted_iota(jnp.int32, (rows, 32), 1)
    slot_t, place_t = t // RLEN, lax.rem(t, RLEN)
    own = (
        (r // RLEN == slot_t)
        & (place_t <= lax.rem(r, RLEN))
        & (place_t < jnp.where(slot_t == 0, len0, len1))
    )
    column = lax.broadcasted_iota(jnp.int32, (rows, 2048), 1)

    def head(h, _):
        lanes = pl.ds(pl.multiple_of(h * HEAD_SIZE, HEAD_SIZE), HEAD_SIZE)
        behind = pl.ds(pl.multiple_of(512 + h * HEAD_SIZE, HEAD_SIZE), HEAD_SIZE)
        heads = [
            pl.ds(pl.multiple_of((h * GROUP + g) * HEAD_SIZE, HEAD_SIZE), HEAD_SIZE) for g in range(GROUP)
        ]
        qs = jnp.concatenate([q[:, at] for at in heads], axis=0)
        s_own = lax.dot_general(qs, rk[:, lanes], ROWS, preferred_element_type=jnp.float32)
        s_own = jnp.where(own, s_own, HIDDEN)
        s = lax.dot_general(qs, kv[:, lanes], ROWS, preferred_element_type=jnp.float32)
        s = jnp.where(column < limit, s, HIDDEN)
        top = jnp.maximum(jnp.max(s, axis=1, keepdims=True), jnp.max(s_own, axis=1, keepdims=True))
        w = jnp.exp2((s - top) * TO_LOG2)
        w_own = jnp.exp2((s_own - top) * TO_LOG2)
        total = jnp.sum(w, axis=1, keepdims=True) + jnp.sum(w_own, axis=1, keepdims=True)
        mixed = jnp.dot(w.astype(jnp.bfloat16), kv[:, behind], preferred_element_type=jnp.float32)
        mixed += jnp.dot(w_own.astype(jnp.bfloat16), rv[:, lanes], preferred_element_type=jnp.float32)
        done = (mixed / total).astype(jnp.bfloat16)
        for g, at in enumerate(heads):
            attn[:, at] = done[g * 32 : (g + 1) * 32, :]
        return 0

    lax.fori_loop(0, KEY_VALUE_HEADS, head, 0)
    stream = resid[...].astype(jnp.float32) + attn[...].astype(jnp.float32)
    scale = lax.rsqrt(jnp.mean(stream * stream, axis=1, keepdims=True) + 1e-05)
    out[...] = (stream * scale * gain[...]).astype(jnp.bfloat16)


def resp_attention(plen, rlen, blocks, q, rk, rv, resid, gain):
    return pl.pallas_call(
        resp_kernel,
        out_shape=(
            jax.ShapeDtypeStruct((2048, 1024), jnp.bfloat16),
            jax.ShapeDtypeStruct((32, 4096), jnp.bfloat16),
        ),
        in_specs=[SMEM, SMEM] + [VMEM] * 11,
        out_specs=(VMEM, VMEM),
        scratch_shapes=[pltpu.VMEM((32, 4096), jnp.bfloat16)],
        compiler_params=params(20),
        cost_estimate=cost(4 * 1024 * 2080 * 128, 9 << 20, 1024 * 2080),
        name="resp_attention",
    )(plen, rlen, *blocks, q, rk, rv, resid, gain)


def prompt_kernel(plen, q, keys, values, *refs):
    out = refs[-1]
    _, _, y, xl, c = places()
    here = (y * 2 + xl) * 2 + c
    rows = 2 * 128
    place = lax.rem(lax.broadcasted_iota(jnp.int32, (rows, 1), 0), 128)
    ends = jnp.minimum(here * 128 + place + 1, plen[0])
    column = lax.broadcasted_iota(jnp.int32, (rows, 2048), 1)

    def two_heads(i, _):
        heads = [pl.ds(pl.multiple_of((i * 2 + g) * HEAD_SIZE, HEAD_SIZE), HEAD_SIZE) for g in range(2)]
        qs = jnp.concatenate([q[:, at] for at in heads], axis=0)
        s = lax.dot_general(qs, keys[...], ROWS, preferred_element_type=jnp.float32)
        s = jnp.where(column < ends, s, HIDDEN)
        top = jnp.max(s, axis=1, keepdims=True)
        w = jnp.exp2((s - top) * TO_LOG2)
        total = jnp.sum(w, axis=1, keepdims=True)
        mixed = jnp.dot(w.astype(jnp.bfloat16), values[...], preferred_element_type=jnp.float32)
        done = (mixed / total).astype(jnp.bfloat16)
        for g, at in enumerate(heads):
            out[:, at] = done[g * 128 : (g + 1) * 128, :]
        return 0

    lax.fori_loop(0, GROUP // 2, two_heads, 0)


def prompt_attention(plen, q, kv, first, count, before):
    return pl.pallas_call(
        prompt_kernel,
        out_shape=jax.ShapeDtypeStruct((128, 4096), jnp.bfloat16),
        grid=(count,),
        in_specs=[
            SMEM,
            pl.BlockSpec((128, 1024), lambda i: (0, i + first)),
            pl.BlockSpec((2048, 128), lambda i: (0, i + first)),
            pl.BlockSpec((2048, 128), lambda i: (0, i + first + KEY_VALUE_HEADS)),
        ]
        + [pl.BlockSpec(memory_space=pl.ANY)] * len(before),
        out_specs=pl.BlockSpec((128, 1024), lambda i: (0, i + first)),
        input_output_aliases={4: 0} if before else {},
        compiler_params=params(16),
        cost_estimate=cost(count * 12 * 1024 * 2048 * 128, count << 20, count * 1024 * 2048),
        name="prompt_attention",
    )(plen, q, kv, kv, *before)


def rows_kernel(*refs):
    blocks, out = refs[:-1], refs[-1]
    xh, _, y, xl, c = places()
    x = xh * 2 + xl
    for side in range(2):
        cc = c if side == 0 else 1 - c
        for part, d in enumerate(RING):
            ref = blocks[side * 4 + part]
            for n, inner in enumerate(RING):
                dx = jnp.where(cc == 0, inner, d)
                dy = jnp.where(cc == 0, d, inner)
                xx, yy = lax.rem(x + dx + 4, 4), lax.rem(y + dy + 4, 4)
                row = (xx // 2) * 512 + yy * 128 + lax.rem(xx, 2) * 64 + cc * 32
                out[pl.ds(pl.multiple_of(row, 32), 32), :] = ref[n * 32 : (n + 1) * 32, :]


def assemble_rows(blocks):
    return pl.pallas_call(
        rows_kernel,
        out_shape=jax.ShapeDtypeStruct((1024, 4096), jnp.bfloat16),
        in_specs=[VMEM] * 8,
        out_specs=VMEM,
        compiler_params=params(24),
        cost_estimate=cost(10**9, 16 << 20),
        name="assemble_rows",
    )(*blocks)


def weights_kernel(*refs):
    (mine, first, second), steps, last, w = refs[:3], refs[3:9], refs[9], refs[10]
    xh, z, _, _, c = places()

    def put(step, other, ref, at):
        half = 1 - xh if other else xh
        from_z = lax.rem(z + jnp.where(c == 0, 8 - step, step), 8)
        w[pl.ds(pl.multiple_of((half * 8 + from_z) * 256, 256), 256), :] = ref[at : at + 256, :]

    put(0, False, mine, 0)
    put(1, False, first, 0)
    put(0, True, second, 0)
    for i, ref in enumerate(steps):
        put(i + 2, False, ref, 0)
        put(i + 1, True, ref, 256)
    put(7, True, last, 0)


def assemble_weights(slices):
    return pl.pallas_call(
        weights_kernel,
        out_shape=jax.ShapeDtypeStruct((4096, 896), jnp.bfloat16),
        in_specs=[VMEM] * 10,
        out_specs=VMEM,
        compiler_params=params(20),
        cost_estimate=cost(10**9, 14 << 20),
        name="assemble_weights",
    )(*slices)


def hidden_kernel(group, a, w, out):
    rows = pl.ds(pl.multiple_of(group[0] * 512, 512), 512)

    def put(lanes, gate, up):
        out[:, lanes] = (gate / (1.0 + jnp.exp(-gate)) * up).astype(jnp.bfloat16)

    def block(b, _):
        cols = pl.ds(pl.multiple_of(b * 256, 256), 256)
        both = jnp.dot(a[rows, :], w[:, cols], preferred_element_type=jnp.float32)
        put(pl.ds(pl.multiple_of(b * 128, 128), 128), both[:, :128], both[:, 128:])
        return 0

    lax.fori_loop(0, 3, block, 0)
    both = jnp.dot(a[rows, :], w[:, 768:896], preferred_element_type=jnp.float32)
    put(slice(384, 448), both[:, :64], both[:, 64:])


def hidden_part(group, a, w):
    return pl.pallas_call(
        hidden_kernel,
        out_shape=jax.ShapeDtypeStruct((512, 448), jnp.bfloat16),
        in_specs=[SMEM, VMEM, VMEM],
        out_specs=VMEM,
        compiler_params=params(24),
        cost_estimate=cost(2 * 512 * 4096 * 896, 12 << 20),
        name="hidden_part",
    )(group, a, w)


def local(
    prompt_q,
    prompt_k,
    prompt_v,
    prompt_len,
    resp_q,
    resp_k,
    resp_v,
    resp_len,
    resp_resid,
    norm_gain,
    gate_weight,
    up_weight,
):
    xh = lax.axis_index("xh").astype(jnp.int32)
    own = jnp.concatenate([prompt_k[0], prompt_v[0]], axis=1)
    pair = jnp.concatenate([own, shift(own, "xl", 1)], axis=0)
    blocks = ring4_halves(pair, "y", along_y)
    blocks = blocks + [shift(jnp.concatenate(blocks[:3], axis=0), "c", 1), shift(blocks[3], "c", 1)]

    mine, theirs = pack(gate_weight, up_weight)
    slices = gather_slices(mine, theirs)

    kv, rows = resp_attention(
        prompt_len,
        resp_len,
        blocks,
        resp_q[0],
        resp_k[0],
        resp_v[0],
        resp_resid[0],
        norm_gain.reshape(1, -1),
    )
    axes = ("xh",) + CTX
    line = jnp.concatenate(ring4(rows, axes, functools.partial(crossed, True)), axis=0)
    plane = ring4(line, axes, functools.partial(crossed, False))
    blocks = shared(plane)
    out = prompt_attention(prompt_len, prompt_q[0], kv, 0, 2, ())

    out = prompt_attention(prompt_len, prompt_q[0], kv, 2, 1, (out,))

    rows = assemble_rows(blocks)
    w = assemble_weights(slices)
    away = hidden_part((1 - xh).reshape(1), rows, w)
    got = shift(away, "xh", 1)
    done = hidden_part(xh.reshape(1), rows, w)
    out = prompt_attention(prompt_len, prompt_q[0], kv, 3, 1, (out,))
    zero = jnp.where(xh == 0, done, got)
    one = jnp.where(xh == 0, got, done)
    hidden = jnp.concatenate([zero, one[:, 384:], one[:, :384]], axis=1)
    return (out[None], hidden[None])


def solution(mesh):
    finer = Mesh(mesh.devices.reshape(2, 8, 4, 2, 2), ("xh", "z", "y", "xl", "c"))

    return jax.shard_map(
        local,
        mesh=finer,
        in_specs=(
            P(DP, CTX, None),
            P(DP, CTX, None),
            P(DP, CTX, None),
            P(DP),
            P(DP, CTX, None),
            P(DP, CTX, None),
            P(DP, CTX, None),
            P(DP, CTX),
            P(DP, CTX, None),
            P(),
            P(DP, CTX),
            P(DP, CTX),
        ),
        out_specs=(P(DP, CTX, None), P(DP, None, CTX)),
        check_vma=False,
    )
```

```python
import functools

import jax
import jax.numpy as jnp
from jax import lax
from jax.experimental import pallas as pl
from jax.experimental.pallas import tpu as pltpu
from jax.sharding import Mesh
from jax.sharding import PartitionSpec as P

KEY_VALUE_HEADS = 4
GROUP = 8
HEAD_SIZE = 128
RLEN = 16
CTX = ("y", "xl", "c")
DP = ("xh", "z")
TO_LOG2 = 1.4426950408889634 * HEAD_SIZE**-0.5
HIDDEN = -1e30
VMEM = pl.BlockSpec(memory_space=pltpu.VMEM)
SMEM = pl.BlockSpec(memory_space=pltpu.SMEM)


def params(limit):
    return pltpu.CompilerParams(vmem_limit_bytes=limit << 20)


def cost(flops, moved, exps=0):
    return pl.CostEstimate(flops=flops, bytes_accessed=moved, transcendentals=exps)


def shift(a, axis, by):
    n = lax.axis_size(axis)
    return lax.ppermute(a, axis, [(i, (i + by) % n) for i in range(n)])


def halves(a, axis):
    n = a.shape[axis] // 2
    return lax.slice_in_dim(a, 0, n, axis=axis), lax.slice_in_dim(a, n, 2 * n, axis=axis)


def ring4(a, axes, pairs):
    return [a] + [lax.ppermute(a, axes, pairs(by)) for by in (1, -1, 2)]


def ring4_halves(a, axes, pairs):
    low = lax.ppermute(a, axes, pairs(1))
    high = lax.ppermute(a, axes, pairs(-1))
    far_a = lax.ppermute(halves(low, 0)[0], axes, pairs(1))
    far_b = lax.ppermute(halves(high, 0)[1], axes, pairs(-1))
    return [a, low, high, jnp.concatenate([far_a, far_b], axis=0)]


def shared(pieces):
    return pieces + [shift(a, "c", 1) for a in pieces]


def along_y(by):
    return [(i, (i + by) % 4) for i in range(4)]


def crossed(x_first, by):
    def flat(x, y, c):
        return ((x // 2 * 4 + y) * 2 + x % 2) * 2 + c

    out = []
    for x in range(4):
        for y in range(4):
            for c in range(2):
                to = ((x + by) % 4, y) if (c == 0) == x_first else (x, (y + by) % 4)
                out.append((flat(x, y, c), flat(*to, c)))
    return out


RING = (0, -1, 1, 2)


def places():
    return [lax.axis_index(a).astype(jnp.int32) for a in ("xh", "z", "y", "xl", "c")]


def pack_kernel(gate, up, mine, theirs):
    xh = places()[0]

    def pack(half, out):
        start, tail = (0, 384) if half == 0 else (512, 448)
        for b in range(3):
            at = start + 128 * b
            out[:, 256 * b : 256 * b + 128] = gate[:, at : at + 128]
            out[:, 256 * b + 128 : 256 * b + 256] = up[:, at : at + 128]
        out[:, 768:832] = gate[:, tail : tail + 64]
        out[:, 832:896] = up[:, tail : tail + 64]

    @pl.when(xh == 0)
    def _():
        pack(0, mine)
        pack(1, theirs)

    @pl.when(xh != 0)
    def _():
        pack(1, mine)
        pack(0, theirs)


def pack(gate, up):
    shape = jax.ShapeDtypeStruct(gate.shape, gate.dtype)
    return pl.pallas_call(
        pack_kernel,
        out_shape=(shape, shape),
        in_specs=[VMEM, VMEM],
        out_specs=(VMEM, VMEM),
        compiler_params=params(8),
        cost_estimate=cost(10**9, 2 * 2 * gate.size * 2),
        name="pack",
    )(gate, up)


def ring8(shard):
    pairs = []
    for z in range(8):
        for c in range(2):
            pairs.append((z * 2 + c, (z + (1, -1)[c]) % 8 * 2 + c))
    pieces = [shard]
    for _ in range(1, 8):
        pieces.append(lax.ppermute(pieces[-1], ("z", "c"), pairs))
    return pieces


ROWS = (((1,), (1,)), ((), ()))


def resp_kernel(plen, rlen, *refs):
    blocks, (q, rk, rv, resid, gain, kv, out, attn) = refs[:6], refs[6:]
    _, _, y, xl, c = places()
    limit, len0, len1 = plen[0], rlen[0, 0], rlen[0, 1]
    for i in range(8):
        cc = c if i < 4 else 1 - c
        ref, at = (blocks[i], 0) if i < 4 else (blocks[4], (i - 4) * 256) if i < 7 else (blocks[5], 0)
        yy = lax.rem(y + RING[i % 4] + 4, 4)
        for beside in range(2):
            xx = xl if beside == 0 else 1 - xl
            row = pl.multiple_of(((yy * 2 + xx) * 2 + cc) * 128, 128)
            kv[pl.ds(row, 128), :] = ref[at + beside * 128 : at + (beside + 1) * 128, :]
    rows = GROUP * 32
    r = lax.rem(lax.broadcasted_iota(jnp.int32, (rows, 32), 0), 32)
    t = lax.broadcasted_iota(jnp.int32, (rows, 32), 1)
    slot_t, place_t = t // RLEN, lax.rem(t, RLEN)
    own = (
        (r // RLEN == slot_t)
        & (place_t <= lax.rem(r, RLEN))
        & (place_t < jnp.where(slot_t == 0, len0, len1))
    )
    column = lax.broadcasted_iota(jnp.int32, (rows, 2048), 1)

    def head(h, _):
        lanes = pl.ds(pl.multiple_of(h * HEAD_SIZE, HEAD_SIZE), HEAD_SIZE)
        behind = pl.ds(pl.multiple_of(512 + h * HEAD_SIZE, HEAD_SIZE), HEAD_SIZE)
        heads = [
            pl.ds(pl.multiple_of((h * GROUP + g) * HEAD_SIZE, HEAD_SIZE), HEAD_SIZE) for g in range(GROUP)
        ]
        qs = jnp.concatenate([q[:, at] for at in heads], axis=0)
        s_own = lax.dot_general(qs, rk[:, lanes], ROWS, preferred_element_type=jnp.float32)
        s_own = jnp.where(own, s_own, HIDDEN)
        s = lax.dot_general(qs, kv[:, lanes], ROWS, preferred_element_type=jnp.float32)
        s = jnp.where(column < limit, s, HIDDEN)
        top = jnp.maximum(jnp.max(s, axis=1, keepdims=True), jnp.max(s_own, axis=1, keepdims=True))
        w = jnp.exp2((s - top) * TO_LOG2)
        w_own = jnp.exp2((s_own - top) * TO_LOG2)
        total = jnp.sum(w, axis=1, keepdims=True) + jnp.sum(w_own, axis=1, keepdims=True)
        mixed = jnp.dot(w.astype(jnp.bfloat16), kv[:, behind], preferred_element_type=jnp.float32)
        mixed += jnp.dot(w_own.astype(jnp.bfloat16), rv[:, lanes], preferred_element_type=jnp.float32)
        done = (mixed / total).astype(jnp.bfloat16)
        for g, at in enumerate(heads):
            attn[:, at] = done[g * 32 : (g + 1) * 32, :]
        return 0

    lax.fori_loop(0, KEY_VALUE_HEADS, head, 0)
    stream = resid[...].astype(jnp.float32) + attn[...].astype(jnp.float32)
    scale = lax.rsqrt(jnp.mean(stream * stream, axis=1, keepdims=True) + 1e-05)
    out[...] = (stream * scale * gain[...]).astype(jnp.bfloat16)


def resp_attention(plen, rlen, blocks, q, rk, rv, resid, gain):
    return pl.pallas_call(
        resp_kernel,
        out_shape=(
            jax.ShapeDtypeStruct((2048, 1024), jnp.bfloat16),
            jax.ShapeDtypeStruct((32, 4096), jnp.bfloat16),
        ),
        in_specs=[SMEM, SMEM] + [VMEM] * 11,
        out_specs=(VMEM, VMEM),
        scratch_shapes=[pltpu.VMEM((32, 4096), jnp.bfloat16)],
        compiler_params=params(20),
        cost_estimate=cost(4 * 1024 * 2080 * 128, 9 << 20, 1024 * 2080),
        name="resp_attention",
    )(plen, rlen, *blocks, q, rk, rv, resid, gain)


def prompt_kernel(plen, q, keys, values, *refs):
    out = refs[-1]
    _, _, y, xl, c = places()
    here = (y * 2 + xl) * 2 + c
    rows = 2 * 128
    place = lax.rem(lax.broadcasted_iota(jnp.int32, (rows, 1), 0), 128)
    ends = jnp.minimum(here * 128 + place + 1, plen[0])
    column = lax.broadcasted_iota(jnp.int32, (rows, 2048), 1)

    def two_heads(i, _):
        heads = [pl.ds(pl.multiple_of((i * 2 + g) * HEAD_SIZE, HEAD_SIZE), HEAD_SIZE) for g in range(2)]
        qs = jnp.concatenate([q[:, at] for at in heads], axis=0)
        s = lax.dot_general(qs, keys[...], ROWS, preferred_element_type=jnp.float32)
        s = jnp.where(column < ends, s, HIDDEN)
        top = jnp.max(s, axis=1, keepdims=True)
        w = jnp.exp2((s - top) * TO_LOG2)
        total = jnp.sum(w, axis=1, keepdims=True)
        mixed = jnp.dot(w.astype(jnp.bfloat16), values[...], preferred_element_type=jnp.float32)
        done = (mixed / total).astype(jnp.bfloat16)
        for g, at in enumerate(heads):
            out[:, at] = done[g * 128 : (g + 1) * 128, :]
        return 0

    lax.fori_loop(0, GROUP // 2, two_heads, 0)


def prompt_attention(plen, q, kv, first, count, before):
    return pl.pallas_call(
        prompt_kernel,
        out_shape=jax.ShapeDtypeStruct((128, 4096), jnp.bfloat16),
        grid=(count,),
        in_specs=[
            SMEM,
            pl.BlockSpec((128, 1024), lambda i: (0, i + first)),
            pl.BlockSpec((2048, 128), lambda i: (0, i + first)),
            pl.BlockSpec((2048, 128), lambda i: (0, i + first + KEY_VALUE_HEADS)),
        ]
        + [pl.BlockSpec(memory_space=pl.ANY)] * len(before),
        out_specs=pl.BlockSpec((128, 1024), lambda i: (0, i + first)),
        input_output_aliases={4: 0} if before else {},
        compiler_params=params(16),
        cost_estimate=cost(count * 12 * 1024 * 2048 * 128, count << 20, count * 1024 * 2048),
        name="prompt_attention",
    )(plen, q, kv, kv, *before)


def rows_kernel(*refs):
    blocks, out = refs[:-1], refs[-1]
    xh, _, y, xl, c = places()
    x = xh * 2 + xl
    for side in range(2):
        cc = c if side == 0 else 1 - c
        for part, d in enumerate(RING):
            ref = blocks[side * 4 + part]
            for n, inner in enumerate(RING):
                dx = jnp.where(cc == 0, inner, d)
                dy = jnp.where(cc == 0, d, inner)
                xx, yy = lax.rem(x + dx + 4, 4), lax.rem(y + dy + 4, 4)
                row = (xx // 2) * 512 + yy * 128 + lax.rem(xx, 2) * 64 + cc * 32
                out[pl.ds(pl.multiple_of(row, 32), 32), :] = ref[n * 32 : (n + 1) * 32, :]


def assemble_rows(blocks):
    return pl.pallas_call(
        rows_kernel,
        out_shape=jax.ShapeDtypeStruct((1024, 4096), jnp.bfloat16),
        in_specs=[VMEM] * 8,
        out_specs=VMEM,
        compiler_params=params(24),
        cost_estimate=cost(10**9, 16 << 20),
        name="assemble_rows",
    )(*blocks)


def weights_kernel(*refs):
    slices, w = refs[:-1], refs[-1]
    xh, z, _, _, c = places()
    for i, ref in enumerate(slices):
        half = xh if i < 8 else 1 - xh
        from_z = lax.rem(z + jnp.where(c == 0, 8 - i % 8, i % 8), 8)
        w[pl.ds(pl.multiple_of((half * 8 + from_z) * 256, 256), 256), :] = ref[...]


def assemble_weights(slices):
    return pl.pallas_call(
        weights_kernel,
        out_shape=jax.ShapeDtypeStruct((4096, 896), jnp.bfloat16),
        in_specs=[VMEM] * 16,
        out_specs=VMEM,
        compiler_params=params(20),
        cost_estimate=cost(10**9, 14 << 20),
        name="assemble_weights",
    )(*slices)


def hidden_kernel(group, a, w, out):
    rows = pl.ds(pl.multiple_of(group[0] * 512, 512), 512)

    def put(lanes, gate, up):
        out[:, lanes] = (gate / (1.0 + jnp.exp(-gate)) * up).astype(jnp.bfloat16)

    def block(b, _):
        cols = pl.ds(pl.multiple_of(b * 256, 256), 256)
        both = jnp.dot(a[rows, :], w[:, cols], preferred_element_type=jnp.float32)
        put(pl.ds(pl.multiple_of(b * 128, 128), 128), both[:, :128], both[:, 128:])
        return 0

    lax.fori_loop(0, 3, block, 0)
    both = jnp.dot(a[rows, :], w[:, 768:896], preferred_element_type=jnp.float32)
    put(slice(384, 448), both[:, :64], both[:, 64:])


def hidden_part(group, a, w):
    return pl.pallas_call(
        hidden_kernel,
        out_shape=jax.ShapeDtypeStruct((512, 448), jnp.bfloat16),
        in_specs=[SMEM, VMEM, VMEM],
        out_specs=VMEM,
        compiler_params=params(24),
        cost_estimate=cost(2 * 512 * 4096 * 896, 12 << 20),
        name="hidden_part",
    )(group, a, w)


def local(
    prompt_q,
    prompt_k,
    prompt_v,
    prompt_len,
    resp_q,
    resp_k,
    resp_v,
    resp_len,
    resp_resid,
    norm_gain,
    gate_weight,
    up_weight,
):
    xh = lax.axis_index("xh").astype(jnp.int32)
    own = jnp.concatenate([prompt_k[0], prompt_v[0]], axis=1)
    pair = jnp.concatenate([own, shift(own, "xl", 1)], axis=0)
    blocks = ring4_halves(pair, "y", along_y)
    blocks = blocks + [shift(jnp.concatenate(blocks[:3], axis=0), "c", 1), shift(blocks[3], "c", 1)]

    mine, theirs = pack(gate_weight, up_weight)
    first = ring8(mine)
    second = ring8(shift(theirs, "xh", 1))

    kv, rows = resp_attention(
        prompt_len,
        resp_len,
        blocks,
        resp_q[0],
        resp_k[0],
        resp_v[0],
        resp_resid[0],
        norm_gain.reshape(1, -1),
    )
    axes = ("xh",) + CTX
    line = jnp.concatenate(ring4(rows, axes, functools.partial(crossed, True)), axis=0)
    plane = ring4(line, axes, functools.partial(crossed, False))
    blocks = shared(plane)
    out = prompt_attention(prompt_len, prompt_q[0], kv, 0, 2, ())

    out = prompt_attention(prompt_len, prompt_q[0], kv, 2, 1, (out,))

    rows = assemble_rows(blocks)
    w = assemble_weights(first + second)
    away = hidden_part((1 - xh).reshape(1), rows, w)
    got = shift(away, "xh", 1)
    done = hidden_part(xh.reshape(1), rows, w)
    out = prompt_attention(prompt_len, prompt_q[0], kv, 3, 1, (out,))
    zero = jnp.where(xh == 0, done, got)
    one = jnp.where(xh == 0, got, done)
    hidden = jnp.concatenate([zero, one[:, 384:], one[:, :384]], axis=1)
    return (out[None], hidden[None])


def solution(mesh):
    finer = Mesh(mesh.devices.reshape(2, 8, 4, 2, 2), ("xh", "z", "y", "xl", "c"))

    return jax.shard_map(
        local,
        mesh=finer,
        in_specs=(
            P(DP, CTX, None),
            P(DP, CTX, None),
            P(DP, CTX, None),
            P(DP),
            P(DP, CTX, None),
            P(DP, CTX, None),
            P(DP, CTX, None),
            P(DP, CTX),
            P(DP, CTX, None),
            P(),
            P(DP, CTX),
            P(DP, CTX),
        ),
        out_specs=(P(DP, CTX, None), P(DP, None, CTX)),
        check_vma=False,
    )
```

```python
import functools

import jax
import jax.numpy as jnp
from jax import lax
from jax.experimental import pallas as pl
from jax.experimental.pallas import tpu as pltpu
from jax.sharding import Mesh
from jax.sharding import PartitionSpec as P

KEY_VALUE_HEADS = 4
GROUP = 8
HEAD_SIZE = 128
RLEN = 16
CTX = ("y", "xl", "c")
DP = ("xh", "z")
TO_LOG2 = 1.4426950408889634 * HEAD_SIZE**-0.5
HIDDEN = -1e30
VMEM = pl.BlockSpec(memory_space=pltpu.VMEM)
SMEM = pl.BlockSpec(memory_space=pltpu.SMEM)


def params(limit):
    return pltpu.CompilerParams(vmem_limit_bytes=limit << 20)


def cost(flops, moved, exps=0):
    return pl.CostEstimate(flops=flops, bytes_accessed=moved, transcendentals=exps)


def shift(a, axis, by):
    n = lax.axis_size(axis)
    return lax.ppermute(a, axis, [(i, (i + by) % n) for i in range(n)])


def halves(a, axis):
    n = a.shape[axis] // 2
    return lax.slice_in_dim(a, 0, n, axis=axis), lax.slice_in_dim(a, n, 2 * n, axis=axis)


def ring4(a, axes, pairs):
    return [a] + [lax.ppermute(a, axes, pairs(by)) for by in (1, -1, 2)]


def ring4_halves(a, axes, pairs):
    low = lax.ppermute(a, axes, pairs(1))
    high = lax.ppermute(a, axes, pairs(-1))
    far_a = lax.ppermute(halves(low, 0)[0], axes, pairs(1))
    far_b = lax.ppermute(halves(high, 0)[1], axes, pairs(-1))
    return [a, low, high, jnp.concatenate([far_a, far_b], axis=0)]


def shared(pieces):
    return pieces + [shift(a, "c", 1) for a in pieces]


def along_y(by):
    return [(i, (i + by) % 4) for i in range(4)]


def crossed(x_first, by):
    def flat(x, y, c):
        return ((x // 2 * 4 + y) * 2 + x % 2) * 2 + c

    out = []
    for x in range(4):
        for y in range(4):
            for c in range(2):
                to = ((x + by) % 4, y) if (c == 0) == x_first else (x, (y + by) % 4)
                out.append((flat(x, y, c), flat(*to, c)))
    return out


RING = (0, -1, 1, 2)


def places():
    return [lax.axis_index(a).astype(jnp.int32) for a in ("xh", "z", "y", "xl", "c")]


def pack_kernel(gate, up, mine, theirs):
    xh = places()[0]

    def pack(half, out):
        start, tail = (0, 384) if half == 0 else (512, 448)
        for b in range(3):
            at = start + 128 * b
            out[:, 256 * b : 256 * b + 128] = gate[:, at : at + 128]
            out[:, 256 * b + 128 : 256 * b + 256] = up[:, at : at + 128]
        out[:, 768:832] = gate[:, tail : tail + 64]
        out[:, 832:896] = up[:, tail : tail + 64]

    @pl.when(xh == 0)
    def _():
        pack(0, mine)
        pack(1, theirs)

    @pl.when(xh != 0)
    def _():
        pack(1, mine)
        pack(0, theirs)


def pack(gate, up):
    shape = jax.ShapeDtypeStruct(gate.shape, gate.dtype)
    return pl.pallas_call(
        pack_kernel,
        out_shape=(shape, shape),
        in_specs=[VMEM, VMEM],
        out_specs=(VMEM, VMEM),
        compiler_params=params(8),
        cost_estimate=cost(10**9, 2 * 2 * gate.size * 2),
        name="pack",
    )(gate, up)


def ring8(shard):
    pairs = []
    for z in range(8):
        for c in range(2):
            pairs.append((z * 2 + c, (z + (1, -1)[c]) % 8 * 2 + c))
    pieces = [shard]
    for _ in range(1, 8):
        pieces.append(lax.ppermute(pieces[-1], ("z", "c"), pairs))
    return pieces


ROWS = (((1,), (1,)), ((), ()))


def resp_kernel(plen, rlen, *refs):
    blocks, (q, rk, rv, resid, gain, kv, out, attn) = refs[:6], refs[6:]
    _, _, y, xl, c = places()
    limit, len0, len1 = plen[0], rlen[0, 0], rlen[0, 1]
    for i in range(8):
        cc = c if i < 4 else 1 - c
        ref, at = (blocks[i], 0) if i < 4 else (blocks[4], (i - 4) * 256) if i < 7 else (blocks[5], 0)
        yy = lax.rem(y + RING[i % 4] + 4, 4)
        for beside in range(2):
            xx = xl if beside == 0 else 1 - xl
            row = pl.multiple_of(((yy * 2 + xx) * 2 + cc) * 128, 128)
            kv[pl.ds(row, 128), :] = ref[at + beside * 128 : at + (beside + 1) * 128, :]
    rows = GROUP * 32
    r = lax.rem(lax.broadcasted_iota(jnp.int32, (rows, 32), 0), 32)
    t = lax.broadcasted_iota(jnp.int32, (rows, 32), 1)
    slot_t, place_t = t // RLEN, lax.rem(t, RLEN)
    own = (
        (r // RLEN == slot_t)
        & (place_t <= lax.rem(r, RLEN))
        & (place_t < jnp.where(slot_t == 0, len0, len1))
    )
    column = lax.broadcasted_iota(jnp.int32, (rows, 2048), 1)

    def head(h, _):
        lanes = pl.ds(pl.multiple_of(h * HEAD_SIZE, HEAD_SIZE), HEAD_SIZE)
        behind = pl.ds(pl.multiple_of(512 + h * HEAD_SIZE, HEAD_SIZE), HEAD_SIZE)
        heads = [
            pl.ds(pl.multiple_of((h * GROUP + g) * HEAD_SIZE, HEAD_SIZE), HEAD_SIZE) for g in range(GROUP)
        ]
        qs = jnp.concatenate([q[:, at] for at in heads], axis=0)
        s_own = lax.dot_general(qs, rk[:, lanes], ROWS, preferred_element_type=jnp.float32)
        s_own = jnp.where(own, s_own, HIDDEN)
        s = lax.dot_general(qs, kv[:, lanes], ROWS, preferred_element_type=jnp.float32)
        s = jnp.where(column < limit, s, HIDDEN)
        top = jnp.maximum(jnp.max(s, axis=1, keepdims=True), jnp.max(s_own, axis=1, keepdims=True))
        w = jnp.exp2((s - top) * TO_LOG2)
        w_own = jnp.exp2((s_own - top) * TO_LOG2)
        total = jnp.sum(w, axis=1, keepdims=True) + jnp.sum(w_own, axis=1, keepdims=True)
        mixed = jnp.dot(w.astype(jnp.bfloat16), kv[:, behind], preferred_element_type=jnp.float32)
        mixed += jnp.dot(w_own.astype(jnp.bfloat16), rv[:, lanes], preferred_element_type=jnp.float32)
        done = (mixed / total).astype(jnp.bfloat16)
        for g, at in enumerate(heads):
            attn[:, at] = done[g * 32 : (g + 1) * 32, :]
        return 0

    lax.fori_loop(0, KEY_VALUE_HEADS, head, 0)
    stream = resid[...].astype(jnp.float32) + attn[...].astype(jnp.float32)
    scale = lax.rsqrt(jnp.mean(stream * stream, axis=1, keepdims=True) + 1e-05)
    out[...] = (stream * scale * gain[...]).astype(jnp.bfloat16)


def resp_attention(plen, rlen, blocks, q, rk, rv, resid, gain):
    return pl.pallas_call(
        resp_kernel,
        out_shape=(
            jax.ShapeDtypeStruct((2048, 1024), jnp.bfloat16),
            jax.ShapeDtypeStruct((32, 4096), jnp.bfloat16),
        ),
        in_specs=[SMEM, SMEM] + [VMEM] * 11,
        out_specs=(VMEM, VMEM),
        scratch_shapes=[pltpu.VMEM((32, 4096), jnp.bfloat16)],
        compiler_params=params(20),
        cost_estimate=cost(4 * 1024 * 2080 * 128, 9 << 20, 1024 * 2080),
        name="resp_attention",
    )(plen, rlen, *blocks, q, rk, rv, resid, gain)


def prompt_kernel(plen, q, kv, *refs, first):
    out = refs[-1]
    h = first + pl.program_id(0)
    keys = kv.at[:, pl.ds(pl.multiple_of(h * HEAD_SIZE, HEAD_SIZE), HEAD_SIZE)]
    values = kv.at[:, pl.ds(pl.multiple_of(512 + h * HEAD_SIZE, HEAD_SIZE), HEAD_SIZE)]
    _, _, y, xl, c = places()
    here = (y * 2 + xl) * 2 + c
    rows = 2 * 128
    place = lax.rem(lax.broadcasted_iota(jnp.int32, (rows, 1), 0), 128)
    ends = jnp.minimum(here * 128 + place + 1, plen[0])
    column = lax.broadcasted_iota(jnp.int32, (rows, 2048), 1)

    def two_heads(i, _):
        heads = [pl.ds(pl.multiple_of((i * 2 + g) * HEAD_SIZE, HEAD_SIZE), HEAD_SIZE) for g in range(2)]
        asked = [pl.ds(pl.multiple_of((h * GROUP + i * 2 + g) * HEAD_SIZE, HEAD_SIZE), HEAD_SIZE) for g in range(2)]
        qs = jnp.concatenate([q[:, at] for at in asked], axis=0)
        s = lax.dot_general(qs, keys[...], ROWS, preferred_element_type=jnp.float32)
        s = jnp.where(column < ends, s, HIDDEN)
        top = jnp.max(s, axis=1, keepdims=True)
        w = jnp.exp2((s - top) * TO_LOG2)
        total = jnp.sum(w, axis=1, keepdims=True)
        mixed = jnp.dot(w.astype(jnp.bfloat16), values[...], preferred_element_type=jnp.float32)
        done = (mixed / total).astype(jnp.bfloat16)
        for g, at in enumerate(heads):
            out[:, at] = done[g * 128 : (g + 1) * 128, :]
        return 0

    lax.fori_loop(0, GROUP // 2, two_heads, 0)


def prompt_attention(plen, q, kv, first, count, before):
    return pl.pallas_call(
        functools.partial(prompt_kernel, first=first),
        out_shape=jax.ShapeDtypeStruct((128, 4096), jnp.bfloat16),
        grid=(count,),
        in_specs=[SMEM, VMEM, VMEM]
        + [pl.BlockSpec(memory_space=pl.ANY)] * len(before),
        out_specs=pl.BlockSpec((128, 1024), lambda i: (0, i + first)),
        input_output_aliases={3: 0} if before else {},
        compiler_params=params(16),
        cost_estimate=cost(count * 12 * 1024 * 2048 * 128, count << 20, count * 1024 * 2048),
        name="prompt_attention",
    )(plen, q, kv, *before)


def rows_kernel(*refs):
    blocks, out = refs[:-1], refs[-1]
    xh, _, y, xl, c = places()
    x = xh * 2 + xl
    for side in range(2):
        cc = c if side == 0 else 1 - c
        for part, d in enumerate(RING):
            ref = blocks[side * 4 + part]
            for n, inner in enumerate(RING):
                dx = jnp.where(cc == 0, inner, d)
                dy = jnp.where(cc == 0, d, inner)
                xx, yy = lax.rem(x + dx + 4, 4), lax.rem(y + dy + 4, 4)
                row = (xx // 2) * 512 + yy * 128 + lax.rem(xx, 2) * 64 + cc * 32
                out[pl.ds(pl.multiple_of(row, 32), 32), :] = ref[n * 32 : (n + 1) * 32, :]


def assemble_rows(blocks):
    return pl.pallas_call(
        rows_kernel,
        out_shape=jax.ShapeDtypeStruct((1024, 4096), jnp.bfloat16),
        in_specs=[VMEM] * 8,
        out_specs=VMEM,
        compiler_params=params(24),
        cost_estimate=cost(10**9, 16 << 20),
        name="assemble_rows",
    )(*blocks)


def weights_kernel(*refs):
    slices, w = refs[:-1], refs[-1]
    xh, z, _, _, c = places()
    for i, ref in enumerate(slices):
        half = xh if i < 8 else 1 - xh
        from_z = lax.rem(z + jnp.where(c == 0, 8 - i % 8, i % 8), 8)
        w[pl.ds(pl.multiple_of((half * 8 + from_z) * 256, 256), 256), :] = ref[...]


def assemble_weights(slices):
    return pl.pallas_call(
        weights_kernel,
        out_shape=jax.ShapeDtypeStruct((4096, 896), jnp.bfloat16),
        in_specs=[VMEM] * 16,
        out_specs=VMEM,
        compiler_params=params(20),
        cost_estimate=cost(10**9, 14 << 20),
        name="assemble_weights",
    )(*slices)


def hidden_kernel(group, a, w, out):
    rows = pl.ds(pl.multiple_of(group[0] * 512, 512), 512)

    def put(lanes, gate, up):
        out[:, lanes] = (gate / (1.0 + jnp.exp(-gate)) * up).astype(jnp.bfloat16)

    def block(b, _):
        cols = pl.ds(pl.multiple_of(b * 256, 256), 256)
        both = jnp.dot(a[rows, :], w[:, cols], preferred_element_type=jnp.float32)
        put(pl.ds(pl.multiple_of(b * 128, 128), 128), both[:, :128], both[:, 128:])
        return 0

    lax.fori_loop(0, 3, block, 0)
    both = jnp.dot(a[rows, :], w[:, 768:896], preferred_element_type=jnp.float32)
    put(slice(384, 448), both[:, :64], both[:, 64:])


def hidden_part(group, a, w):
    return pl.pallas_call(
        hidden_kernel,
        out_shape=jax.ShapeDtypeStruct((512, 448), jnp.bfloat16),
        in_specs=[SMEM, VMEM, VMEM],
        out_specs=VMEM,
        compiler_params=params(24),
        cost_estimate=cost(2 * 512 * 4096 * 896, 12 << 20),
        name="hidden_part",
    )(group, a, w)


def local(
    prompt_q,
    prompt_k,
    prompt_v,
    prompt_len,
    resp_q,
    resp_k,
    resp_v,
    resp_len,
    resp_resid,
    norm_gain,
    gate_weight,
    up_weight,
):
    xh = lax.axis_index("xh").astype(jnp.int32)
    own = jnp.concatenate([prompt_k[0], prompt_v[0]], axis=1)
    pair = jnp.concatenate([own, shift(own, "xl", 1)], axis=0)
    blocks = ring4_halves(pair, "y", along_y)
    blocks = blocks + [shift(jnp.concatenate(blocks[:3], axis=0), "c", 1), shift(blocks[3], "c", 1)]

    mine, theirs = pack(gate_weight, up_weight)
    first = ring8(mine)
    second = ring8(shift(theirs, "xh", 1))

    kv, rows = resp_attention(
        prompt_len,
        resp_len,
        blocks,
        resp_q[0],
        resp_k[0],
        resp_v[0],
        resp_resid[0],
        norm_gain.reshape(1, -1),
    )
    axes = ("xh",) + CTX
    line = jnp.concatenate(ring4(rows, axes, functools.partial(crossed, True)), axis=0)
    plane = ring4(line, axes, functools.partial(crossed, False))
    blocks = shared(plane)
    out = prompt_attention(prompt_len, prompt_q[0], kv, 0, 2, ())

    out = prompt_attention(prompt_len, prompt_q[0], kv, 2, 1, (out,))

    rows = assemble_rows(blocks)
    w = assemble_weights(first + second)
    away = hidden_part((1 - xh).reshape(1), rows, w)
    got = shift(away, "xh", 1)
    done = hidden_part(xh.reshape(1), rows, w)
    out = prompt_attention(prompt_len, prompt_q[0], kv, 3, 1, (out,))
    zero = jnp.where(xh == 0, done, got)
    one = jnp.where(xh == 0, got, done)
    hidden = jnp.concatenate([zero, one[:, 384:], one[:, :384]], axis=1)
    return (out[None], hidden[None])


def solution(mesh):
    finer = Mesh(mesh.devices.reshape(2, 8, 4, 2, 2), ("xh", "z", "y", "xl", "c"))

    return jax.shard_map(
        local,
        mesh=finer,
        in_specs=(
            P(DP, CTX, None),
            P(DP, CTX, None),
            P(DP, CTX, None),
            P(DP),
            P(DP, CTX, None),
            P(DP, CTX, None),
            P(DP, CTX, None),
            P(DP, CTX),
            P(DP, CTX, None),
            P(),
            P(DP, CTX),
            P(DP, CTX),
        ),
        out_specs=(P(DP, CTX, None), P(DP, None, CTX)),
        check_vma=False,
    )
```
